32 devices in a mesh: sky: 2 (over y), ma: 4 (over z), freq: 2 (over x), pol: 2 (over core).
Axes of the slice: x: 2, y: 2, z: 4, core: 2. Of those that a mesh axis runs over, the one named last changes fastest.
Arguments:
- alm: bfloat16 [2, 2, 1024, 4, 1024], P(None, 'freq', ('ma', 'pol'), None, 'sky'), parts along dimension 4, may hold values from -6 to 6
- beam: bfloat16 [4, 2, 2, 1024, 1024], P('ma', 'freq', None, 'pol'), may hold values from -0.1875 to 0.1875
- m_table: int32 [4], P('ma'), may hold values from 0 to 511, as said below
- chan_mask: int32 [2], P('freq'), may hold values from 0 to 1, as said below
- noise: float32 [2, 1024], P('freq', 'pol'), may hold values from 0.5 to 4
Outputs:
- scaled: bfloat16 [2, 2, 4, 1024, 1024], P(None, 'freq', 'ma', 'pol', 'sky'), parts along dimension 4
- channel_power: float32 [4], P(('sky', 'freq')), parts along dimension 0
The draws below stay inside these ranges and needn't reach their ends.
There are 2 independent parts, one for each index of `sky`. The reference program is written for one: setup_inputs(seed, part) draws one part's arguments, and reference() takes and returns one part's arrays. A program takes and returns all parts, laid end to end along the dimension named above; an argument that names none is the same for every part. Nothing has to cross between parts.
Inputs may be any that keep to these rules, and one draw needn't show every extreme that they name: `m_table`: the 4 values are distinct whole numbers below 512. `chan_mask`: at least one of the 2 channels is usable.
All inputs are finite; a program needn't handle non-finite values.
Results may differ from the reference program's by a relative error of at most 0.00055.
Values may be sent and summed in bfloat16 or wider, within the bound.
A program may use at most 64 MiB of HBM per device.

```python
import math
import jax
import jax.numpy as jnp
from jax import lax

L = 1024
K = 1024
S = 512
M = 4
F = 2


def draw_m_table(key, part):
    return jax.random.permutation(key, L // 2)[:M].astype(jnp.int32)


def draw_chan_mask(key, part):
    mask_key = jax.random.fold_in(key, 23)
    first_key, second_key = jax.random.split(mask_key)
    flags = (jax.random.randint(first_key, (F,), 0, 4) < 3).astype(jnp.int32)
    chosen = jax.random.randint(second_key, (), 0, F)
    forced = (jnp.arange(F, dtype=jnp.int32) == chosen).astype(jnp.int32)
    return jnp.maximum(flags, forced).astype(jnp.int32)


def block_scale(stream_key, shape, pieces, least, top_value):
    loudness, own = 1.0, jax.random.fold_in(stream_key, 6)
    for dim, parts in pieces:
        draws = jnp.exp(jax.random.uniform(jax.random.fold_in(own, dim), (parts,), jnp.float32, least / len(pieces), top_value / len(pieces)))
        loudness = loudness * jnp.repeat(draws, shape[dim] // parts).reshape([-1 if axis == dim else 1 for axis in range(len(shape))])
    return loudness


def scatter_about(rng, dims, spread, reach, shards=(), held_as=jnp.bfloat16):
    result = spread * jax.random.normal(rng, dims, jnp.float32)
    if shards:
        result = result * block_scale(rng, dims, shards, -0.22, 0.18)
    return jnp.clip(result, -reach, reach).astype(held_as)


def setup_inputs(seed: int = 0, part: int = 0) -> dict:
    key_of = jax.random.split(jax.random.key(seed), 6)
    part_keys = jax.random.split(jax.random.fold_in(key_of[5], part), 6)
    return {
        "alm": scatter_about(part_keys[0], (2, F, L, M, S), 1.0, 6.0, ((1, 2), (2, 8))),
        "beam": scatter_about(key_of[1], (M, F, 2, K, L), L ** -0.5, 0.1875, ((0, 4), (1, 2), (3, 2))),
        "m_table": draw_m_table(jax.random.fold_in(key_of[5], 71), part),
        "chan_mask": draw_chan_mask(jax.random.fold_in(key_of[5], 71), part),
        "noise": jnp.clip(jnp.exp(math.log(4.0) - 2.0794415 * jax.random.uniform(key_of[4], (F, K), jnp.float32) ** block_scale(key_of[4], (F, K), ((0, 2), (1, 2)), -0.2, 0.2)), 0.5, 4.0),
    }


def reference(alm, beam, m_table, chan_mask, noise):
    degree = jnp.arange(L, dtype=jnp.int32)

    def one_mode(inputs):
        response, coeffs, m_value = inputs
        keep_mask = (degree >= m_value)[None, None, :, None]
        active = jnp.where(keep_mask, coeffs, jnp.zeros((), coeffs.dtype)).astype(jnp.float32)
        response = response.astype(jnp.float32)
        real_part = jnp.einsum('fkl,fls->fks', response[:, 0], active[0]) - jnp.einsum('fkl,fls->fks', response[:, 1], active[1])
        imag_part = jnp.einsum('fkl,fls->fks', response[:, 0], active[1]) + jnp.einsum('fkl,fls->fks', response[:, 1], active[0])
        return jnp.stack([real_part, imag_part])
    per_mode = lax.map(one_mode, (beam, jnp.moveaxis(alm, 3, 0), m_table))
    visibility = jnp.transpose(per_mode, (1, 2, 0, 3, 4))
    weighted = visibility * visibility / noise[None, :, None, :, None]
    channel_power = lax.optimization_barrier(jnp.sum(weighted, axis=(0, 2, 3, 4))) / jnp.float32(M * K * S)
    mask_float = chan_mask.astype(jnp.float32)
    live_count = jnp.sum(mask_float)
    band_power = jnp.sum(mask_float * channel_power) / live_count
    factor = mask_float / jnp.sqrt(0.5 * channel_power + 0.5 * band_power + 1e-06)
    scaled = visibility * (lax.rsqrt(noise) * factor[:, None])[None, :, None, :, None]
    return (scaled.astype(jnp.bfloat16), channel_power)
```

```python
import contextlib
import functools

import jax
import jax.numpy as jnp
from jax import lax
from jax.experimental import pallas as pl
from jax.experimental.pallas import tpu as pltpu
from jax.sharding import PartitionSpec as P

MESH = pl.DeviceIdType.MESH
LANES = 128


def mark(name):
    return contextlib.nullcontext()


def across(n, i):
    return n // 2 if 2 * i < n else n // 2 - 1


def processing_order(n, i):
    last = across(n, i)
    rest = sorted((j for j in range(n) if j not in (i, last)), key=lambda j: (-abs(j - i), j))
    return rest + ([last] if last != i else [])


def far_first(n, i):
    return sorted((j for j in range(n) if j != i), key=lambda j: (-abs(j - i), j))


def pick_by(me, values):
    pick = jnp.int32(values[0])
    for i in range(1, len(values)):
        pick = jnp.where(me == i, jnp.int32(values[i]), pick)
    return pick


def step_kernel(
    sizes, total, alm_hbm, beam_hbm, m_hbm, mask_hbm, noise_hbm, acc, scale_ref, power_ref,
    staged, planes, recv, wide, beam_v, inv_n, rs_n, mine, slots, m_ref, mask_ref, noise_ref,
    z_send, z_recv, p_send, p_recv, in_sem, beam_sem, q_send, q_recv, chain, meet, small_sem,
):
    n_ma, n_freq, n_pol = sizes
    n_all = n_ma * n_freq * n_pol
    ma, freq, pol = lax.axis_index("ma"), lax.axis_index("freq"), lax.axis_index("pol")
    block = staged.shape[1]
    groups, splits, _, rows, lanes = recv.shape
    per_source = n_pol * block
    per_group = rows // per_source
    modes = beam_hbm.shape[1]
    my_slot = (freq * n_ma + ma) * n_pol + pol
    few = n_ma <= 8 and per_group == 1

    def place(slot):
        return {"ma": lax.rem(slot // n_pol, n_ma), "freq": slot // (n_pol * n_ma), "pol": lax.rem(slot, n_pol)}

    def loop(low, high, body, unroll=False):
        if unroll:
            for r in range(low, high):
                body(r)
        else:
            lax.fori_loop(low, high, lambda r, _: (body(r), 0)[1], 0)

    def for_peers(body):
        loop(1, n_all, body, n_all <= 32)

    barrier = pltpu.get_barrier_semaphore()

    def tell_line(sem):
        @pl.when(ma > 0)
        def _():
            pl.semaphore_signal(sem, inc=1, device_id={"ma": ma - 1}, device_id_type=MESH)

        @pl.when(ma < n_ma - 1)
        def _():
            pl.semaphore_signal(sem, inc=1, device_id={"ma": ma + 1}, device_id_type=MESH)

    def tell(axis, me, n, sem):
        for q in range(1, n):
            pl.semaphore_signal(sem, inc=1, device_id={axis: lax.rem(me + q, n)}, device_id_type=MESH)

    beside = jnp.where(ma > 0, 1, 0) + jnp.where(ma < n_ma - 1, 1, 0)
    tell_line(barrier)
    tell("pol", pol, n_pol, barrier)
    tell("freq", freq, n_freq, barrier)

    pieces = in_sem.shape[1]
    size = block // pieces
    loads = [
        [pltpu.make_async_copy(
            alm_hbm.at[c, pl.ds(h * size, size)], staged.at[c, pl.ds(h * size, size)], in_sem.at[c, h])
         for h in range(pieces)] for c in range(2)
    ]
    for h in range(pieces):
        for c in range(2):
            loads[c][h].start()
    small = [
        pltpu.make_async_copy(src, dst, small_sem.at[i])
        for i, (src, dst) in enumerate(((m_hbm, m_ref), (mask_hbm, mask_ref), (noise_hbm, noise_ref)))
    ]
    for copy in small:
        copy.start()
    beam_copy = pltpu.make_async_copy(beam_hbm, beam_v, beam_sem)
    beam_copy.start()

    def part(source, core, j):
        start = lax.rem(source, per_group) * per_source + core * block
        return recv.at[source // per_group, j, :, pl.ds(pl.multiple_of(start, block), block)]

    step = min(size, 16)
    for h in range(pieces):
        for c in range(2):
            loads[c][h].wait()
            for e in range(h * size, (h + 1) * size, step):
                turned = jnp.transpose(staged[c, e:e + step], (1, 0, 2))
                for j in range(splits):
                    planes[:, j, c, e:e + step, :] = turned[:, :, j * lanes:(j + 1) * lanes]

    with mark("barrier"):
        pl.semaphore_wait(barrier, beside + n_pol - 1 + n_freq - 1)

    def send(target, j):
        return pltpu.make_async_remote_copy(
            src_ref=planes.at[target, j], dst_ref=part(ma, pol, j),
            send_sem=z_send.at[target, j], recv_sem=z_recv.at[ma, j],
            device_id={"ma": target}, device_id_type=MESH)

    def arrival(source, j):
        return pltpu.make_async_remote_copy(
            src_ref=planes.at[source, j], dst_ref=part(source, pol, j),
            send_sem=z_send.at[source, j], recv_sem=z_recv.at[source, j],
            device_id={"ma": source}, device_id_type=MESH)

    def hop(source, j, q, src):
        return pltpu.make_async_remote_copy(
            src_ref=src, dst_ref=part(source, pol, j),
            send_sem=p_send.at[source, j], recv_sem=p_recv.at[source, j],
            device_id={"pol": lax.rem(pol + q, n_pol)}, device_id_type=MESH)

    def relay(source, j, src=None):
        for q in range(1, n_pol):
            hop(source, j, q, part(source, pol, j) if src is None else src).start()

    def relayed(source, j):
        for q in range(1, n_pol):
            pltpu.make_async_remote_copy(
                src_ref=part(source, pol, j), dst_ref=part(source, lax.rem(pol + q, n_pol), j),
                send_sem=p_send.at[source, j], recv_sem=p_recv.at[source, j],
                device_id={"pol": lax.rem(pol + q, n_pol)}, device_id_type=MESH).wait_recv()

    early = {}
    if few:
        for i in range(n_ma):
            first = [(t, 0) for t in far_first(n_ma, i) if abs(t - i) == 1]
            later = [(t, j) for t in far_first(n_ma, i) for j in range(splits) if (t, j) not in first]
            early[i] = (first, later, max(i, n_ma - 1 - i) - 1)

    def send_phase(phase):
        for i in range(n_ma):
            first, later, when = early[i]
            now = (first if phase == 0 else []) + (later if phase == when else [])
            if now:
                @pl.when(ma == i)
                def _():
                    for t, j in now:
                        send(t, j).start()

    if few:
        send_phase(0)
    for t in range(n_ma - 2):
        tell_line(chain.at[t])
        pl.semaphore_wait(chain.at[t], beside)
        if few:
            send_phase(t + 1)
    if not few:
        for j in range(splits):
            loop(1, n_ma, lambda q: send(lax.rem(ma + q, n_ma), j).start())

    for j in range(splits):
        relay(ma, j, planes.at[ma, j])
        for c in range(2):
            part(ma, pol, j)[c] = planes[ma, j, c]

    for copy in small:
        copy.wait()
    spread = jnp.transpose(jnp.broadcast_to(noise_ref[...], (LANES, modes)))
    inv_n[...] = 1.0 / spread
    rs_n[...] = lax.rsqrt(spread)
    mine[1:2, :] = jnp.full((1, LANES), mask_ref[0, 0].astype(jnp.float32))
    beam_copy.wait()
    strip = min(modes, 128)

    def widen(i):
        k0 = pl.multiple_of(i * strip, strip)
        for g in range(groups):
            degree = lax.broadcasted_iota(jnp.int32, (strip, rows), 1) + g * rows
            keep = degree >= m_ref[0, 0]
            zero = jnp.zeros((strip, rows), jnp.float32)
            b0 = jnp.where(keep, beam_v[0, pl.ds(k0, strip), g * rows:(g + 1) * rows].astype(jnp.float32), zero)
            b1 = jnp.where(keep, beam_v[1, pl.ds(k0, strip), g * rows:(g + 1) * rows].astype(jnp.float32), zero)
            wide[g, pl.ds(k0, strip), 0:rows] = b0.astype(wide.dtype)
            wide[g, pl.ds(k0, strip), rows:2 * rows] = (-b1).astype(wide.dtype)
            wide[g, pl.ds(modes + k0, strip), 0:rows] = b1.astype(wide.dtype)
            wide[g, pl.ds(modes + k0, strip), rows:2 * rows] = b0.astype(wide.dtype)

    with mark("widen"):
        loop(0, modes // strip, widen)
    tell("pol", pol, n_pol, meet.at[0])
    pl.semaphore_wait(meet.at[0], n_pol - 1)
    tell("freq", freq, n_freq, meet.at[1])
    pl.semaphore_wait(meet.at[1], n_freq - 1)

    def product(g, j, k0, core=None):
        if core is None:
            return jnp.dot(wide[g, pl.ds(k0, modes), :], recv[g, j].reshape(2 * rows, lanes),
                           preferred_element_type=jnp.float32)
        start = pl.multiple_of(core * block, block)
        left = jnp.concatenate([wide[g, pl.ds(k0, modes), pl.ds(pl.multiple_of(c * rows + start, block), block)]
                                for c in range(2)], axis=1)
        right = jnp.concatenate([recv[g, j, c, pl.ds(start, block), :] for c in range(2)], axis=0)
        return jnp.dot(left, right, preferred_element_type=jnp.float32)

    def add(g, j, first=False, core=None):
        def body(i):
            k0 = pl.multiple_of(i * modes, modes)
            at = (pl.ds(k0, modes), slice(j * lanes, (j + 1) * lanes))
            value = product(g, j, k0, core)
            acc[at] = value if first else acc[at] + value
        loop(0, 2, body)

    def finish(g, j, power, core=None):
        def body(i, power):
            k0 = pl.multiple_of(i * modes, modes)
            at = (pl.ds(k0, modes), slice(j * lanes, (j + 1) * lanes))
            value = acc[at]
            if g is not None:
                value = value + product(g, j, k0, core)
                acc[at] = value
            weighted = value * value * inv_n[...]
            return power + jnp.sum(weighted.reshape(modes // 8, 8, lanes), axis=0)
        return lax.fori_loop(0, 2, body, power)

    power = jnp.zeros((8, lanes), jnp.float32)
    if few:
        split_last = n_pol == 2
        order = [pick_by(ma, [processing_order(n_ma, i)[k] for i in range(n_ma)]) for k in range(n_ma - 1)]
        with mark("own"):
            for j in range(splits):
                relayed(ma, j)
                add(ma, j, first=True)
        steps = [(k, j) for k in range(n_ma - 1) for j in range(splits)]

        def settle(k, j, power):
            with mark(f"relay{k}_{j}"):
                relayed(order[k], j)
            if k < n_ma - 2:
                add(order[k], j)
                return power
            return finish(order[k], j, power)

        for s, (k, j) in enumerate(steps):
            with mark(f"wait{k}_{j}"):
                arrival(order[k], j).wait_recv()
            relay(order[k], j)
            if s:
                power = settle(*steps[s - 1], power)
        k, j = steps[-1]
        if split_last:
            add(order[k], j, core=pol)
            with mark("relaylast"):
                relayed(order[k], j)
            power = finish(order[k], j, power, core=1 - pol)
        else:
            power = settle(k, j, power)
    else:
        for j in range(splits):
            def pass_on(q):
                source = lax.rem(ma + q, n_ma)
                arrival(source, j).wait_recv()
                relay(source, j)
            loop(1, n_ma, pass_on)
        for j in range(splits):
            loop(0, n_ma, lambda source: relayed(source, j))
            for g in range(groups):
                add(g, j, first=g == 0)
            power = finish(None, j, power)

    row = jnp.sum(power, axis=0, keepdims=True)
    mine[0:1, :] = row
    slots[my_slot, 0:1, :] = row
    slots[my_slot, 1:2, :] = mine[1:2, :]

    def report(r):
        return pltpu.make_async_remote_copy(
            src_ref=mine, dst_ref=slots.at[my_slot], send_sem=q_send.at[r - 1], recv_sem=q_recv.at[my_slot],
            device_id=place(lax.rem(my_slot + r, n_all)), device_id_type=MESH)

    def heard(r):
        source = lax.rem(my_slot + r, n_all)
        pltpu.make_async_remote_copy(
            src_ref=mine, dst_ref=slots.at[source], send_sem=q_send.at[r - 1], recv_sem=q_recv.at[source],
            device_id=place(source), device_id_type=MESH).wait_recv()

    for_peers(lambda r: report(r).start())

    with mark("drain"):
        for j in range(splits):
            loop(1, n_ma, lambda q: send(lax.rem(ma + q, n_ma), j).wait_send(), few)

            def passed(source):
                for q in range(1, n_pol):
                    hop(source, j, q, part(source, pol, j)).wait_send()
            loop(0, n_ma, passed, few)
    with mark("heard"):
        for_peers(heard)

    per_freq = n_ma * n_pol
    masked, live, here = 0.0, 0.0, 0.0
    for f in range(n_freq):
        channel = jnp.sum(jnp.sum(slots[f * per_freq:(f + 1) * per_freq, 0, :], axis=0, keepdims=True), axis=1, keepdims=True) / total
        flag = slots[f * per_freq, 1:2, 0:1]
        masked += flag * channel
        live += flag
        here += jnp.where(freq == f, channel, 0.0)
    band = masked / live
    factor = mine[1:2, 0:1] / jnp.sqrt(0.5 * here + 0.5 * band + 1e-06)
    power_ref[...] = jnp.broadcast_to(here, power_ref.shape)
    scale_ref[...] = rs_n[...] * factor
    for_peers(lambda r: report(r).wait_send())


def rescale_kernel(acc, scale_ref, power_ref, out_ref, channel_ref, staged, channel, sems, channel_sem):
    modes = scale_ref.shape[0]
    columns = acc.shape[1]
    strip = modes // sems.shape[0]
    channel[0] = power_ref[0, 0]
    last = pltpu.make_async_copy(channel, channel_ref, channel_sem)
    copies = []
    for i in range(sems.shape[0]):
        k0 = i * strip
        scale = scale_ref[k0:k0 + strip, :]
        for c in range(2):
            for j in range(columns // LANES):
                value = acc[c * modes + k0:c * modes + k0 + strip, j * LANES:(j + 1) * LANES]
                staged[c, k0:k0 + strip, j * LANES:(j + 1) * LANES] = (value * scale).astype(staged.dtype)
        copies.append(pltpu.make_async_copy(
            staged.at[:, pl.ds(k0, strip)], out_ref.at[:, pl.ds(k0, strip)], sems.at[i]))
        copies[-1].start()
        if i == 0:
            last.start()
    for copy in copies:
        copy.wait()
    last.wait()


def on_device(sizes, alm, beam, m_table, chan_mask, noise):
    n_ma, n_freq, n_pol = sizes
    coeffs = alm[:, 0]
    response = beam[0, 0]
    block, columns = coeffs.shape[1], coeffs.shape[3]
    modes, degrees = response.shape[1], response.shape[2]
    per_source = n_pol * block
    rows = per_source * max(1, min(n_ma, 256 // per_source))
    groups = degrees // rows
    splits = columns // LANES
    n_all = n_ma * n_freq * n_pol
    total = float(n_ma * modes * n_pol * columns)
    vmem = pl.BlockSpec(memory_space=pltpu.VMEM)
    hbm = pl.BlockSpec(memory_space=pltpu.HBM)
    dma = pltpu.SemaphoreType.DMA
    keep = functools.partial(pltpu.with_memory_space_constraint, memory_space=pltpu.HBM)
    visibility, scale, power = pl.pallas_call(
        functools.partial(step_kernel, sizes, total),
        out_shape=(
            jax.ShapeDtypeStruct((2 * modes, columns), jnp.float32),
            jax.ShapeDtypeStruct((modes, LANES), jnp.float32),
            jax.ShapeDtypeStruct((1, LANES), jnp.float32),
        ),
        in_specs=[hbm, hbm, hbm, hbm, hbm],
        out_specs=(vmem, vmem, vmem),
        scratch_shapes=[
            pltpu.VMEM((2, block, n_ma, columns), jnp.bfloat16),
            pltpu.VMEM((n_ma, splits, 2, block, LANES), jnp.bfloat16),
            pltpu.VMEM((groups, splits, 2, rows, LANES), jnp.bfloat16),
            pltpu.VMEM((groups, 2 * modes, 2 * rows), jnp.bfloat16),
            pltpu.VMEM((2, modes, degrees), jnp.bfloat16),
            pltpu.VMEM((modes, LANES), jnp.float32),
            pltpu.VMEM((modes, LANES), jnp.float32),
            pltpu.VMEM((2, LANES), jnp.float32),
            pltpu.VMEM((n_all, 2, LANES), jnp.float32),
            pltpu.SMEM((1, 1), jnp.int32),
            pltpu.SMEM((1, 1), jnp.int32),
            pltpu.VMEM((1, modes), jnp.float32),
            dma((n_ma, splits)), dma((n_ma, splits)), dma((n_ma, splits)), dma((n_ma, splits)),
            dma((2, 2 if block % 32 == 0 else 1)), dma,
            dma((n_all,)), dma((n_all,)),
            pltpu.SemaphoreType.REGULAR((max(1, n_ma - 2),)), pltpu.SemaphoreType.REGULAR((2,)), dma((3,)),
        ],
        compiler_params=pltpu.CompilerParams(collective_id=0, has_side_effects=True, vmem_limit_bytes=40 * 1024 * 1024),
        name="driftscan_step",
    )(keep(coeffs), keep(response), m_table[None], chan_mask[None], keep(noise))
    pieces = 8 if modes % 128 == 0 else 1
    scaled, channel_power = pl.pallas_call(
        rescale_kernel,
        out_shape=(
            jax.ShapeDtypeStruct((2, modes, columns), jnp.bfloat16),
            jax.ShapeDtypeStruct((1,), jnp.float32),
        ),
        in_specs=[vmem, vmem, vmem],
        out_specs=(hbm, hbm),
        scratch_shapes=[pltpu.VMEM((2, modes, columns), jnp.bfloat16), pltpu.SMEM((1,), jnp.float32), dma((pieces,)), dma],
        compiler_params=pltpu.CompilerParams(vmem_limit_bytes=16 * 1024 * 1024),
        name="rescale",
    )(visibility, scale, power)
    return scaled[:, None, None], channel_power


def solution(mesh):
    sizes = (mesh.shape["ma"], mesh.shape["freq"], mesh.shape["pol"])
    return jax.shard_map(
        functools.partial(on_device, sizes),
        mesh=mesh,
        in_specs=(
            P(None, "freq", ("ma", "pol"), None, "sky"),
            P("ma", "freq", None, "pol", None),
            P("ma"),
            P("freq"),
            P("freq", "pol"),
        ),
        out_specs=(P(None, "freq", "ma", "pol", "sky"), P(("sky", "freq"))),
        check_vma=False,
    )
```

```python
import contextlib
import functools

import jax
import jax.numpy as jnp
from jax import lax
from jax.experimental import pallas as pl
from jax.experimental.pallas import tpu as pltpu
from jax.sharding import PartitionSpec as P

MESH = pl.DeviceIdType.MESH
LANES = 128


def mark(name):
    return contextlib.nullcontext()


def across(n, i):
    return n // 2 if 2 * i < n else n // 2 - 1


def processing_order(n, i):
    last = across(n, i)
    rest = sorted((j for j in range(n) if j not in (i, last)), key=lambda j: (-abs(j - i), j))
    return rest + ([last] if last != i else [])


def far_first(n, i):
    return sorted((j for j in range(n) if j != i), key=lambda j: (-abs(j - i), j != across(n, i), j))


def pick_by(me, values):
    pick = jnp.int32(values[0])
    for i in range(1, len(values)):
        pick = jnp.where(me == i, jnp.int32(values[i]), pick)
    return pick


def step_kernel(
    sizes, total, alm_hbm, beam_hbm, m_ref, mask_ref, noise_hbm, acc, scale_ref, power_ref,
    staged, planes, recv, wide, beam_v, inv_n, rs_n, mine, slots, noise_ref,
    z_send, z_far, z_last, d_send, p_send, p_far, p_last, in_sem, beam_sem, q_send, q_recv, edge, meet, small_sem,
):
    n_ma, n_freq, n_pol = sizes
    n_all = n_ma * n_freq * n_pol
    ma, freq, pol = lax.axis_index("ma"), lax.axis_index("freq"), lax.axis_index("pol")
    block = staged.shape[1]
    groups, splits, _, rows, lanes = recv.shape
    per_source = n_pol * block
    per_group = rows // per_source
    modes = beam_hbm.shape[1]
    my_slot = (freq * n_ma + ma) * n_pol + pol
    few = n_ma <= 8 and per_group == 1 and n_pol == 2 and block % LANES == 0

    def place(slot):
        return {"ma": lax.rem(slot // n_pol, n_ma), "freq": slot // (n_pol * n_ma), "pol": lax.rem(slot, n_pol)}

    def loop(low, high, body, unroll=False):
        if unroll:
            for r in range(low, high):
                body(r)
        else:
            lax.fori_loop(low, high, lambda r, _: (body(r), 0)[1], 0)

    def for_peers(body):
        loop(1, n_all, body, n_all <= 32)

    barrier = pltpu.get_barrier_semaphore()

    def tell(axis, me, n, sem):
        loop(1, n, lambda q: pl.semaphore_signal(
            sem, inc=1, device_id={axis: lax.rem(me + q, n)}, device_id_type=MESH), n <= 8)

    low = n_ma // 2
    below = ma < low
    inward, outward = jnp.where(below, ma + 1, ma - 1), jnp.where(below, ma - 1, ma + 1)
    is_hub = jnp.logical_or(ma == low - 1, ma == low)
    has_outward = jnp.logical_and(ma > 0, ma < n_ma - 1)

    def tell_line(there, sem):
        pl.semaphore_signal(sem, inc=1, device_id={"ma": there}, device_id_type=MESH)

    @pl.when(is_hub)
    def _():
        tell_line(inward, barrier)

    @pl.when(has_outward)
    def _():
        tell_line(outward, barrier)

    tell("pol", pol, n_pol, barrier)
    tell("freq", freq, n_freq, barrier)

    pieces = in_sem.shape[0]
    width = splits // pieces

    def columns_of(h):
        return pl.ds(h * width * lanes, width * lanes)

    loads = [pltpu.make_async_copy(alm_hbm.at[:, :, :, columns_of(h)], staged.at[:, :, :, columns_of(h)], in_sem.at[h])
             for h in range(pieces)]
    for load in loads:
        load.start()
    noise_copy = pltpu.make_async_copy(noise_hbm, noise_ref, small_sem)
    beam_copy = pltpu.make_async_copy(beam_hbm, beam_v, beam_sem)

    def part(source, core, j):
        start = lax.rem(source, per_group) * per_source + core * block
        return recv.at[source // per_group, j, :, pl.ds(pl.multiple_of(start, block), block)]

    with mark("barrier"):
        pl.semaphore_wait(barrier, 1 + n_pol - 1 + n_freq - 1)

    @pl.when(jnp.logical_not(jnp.logical_or(is_hub, has_outward)))
    def _():
        tell_line(inward, edge.at[0])

    step = min(block, 16)

    def turn(h):
        with mark("load"):
            loads[h].wait()
        for c in range(2):
            for e in range(0, block, step):
                turned = jnp.transpose(staged[c, e:e + step, :, columns_of(h)], (1, 0, 2))
                for j in range(width):
                    planes[:, h * width + j, c, e:e + step, :] = turned[:, :, j * lanes:(j + 1) * lanes]

    def push(src, dst, sent, got, where):
        pltpu.make_async_remote_copy(
            src_ref=src, dst_ref=dst, send_sem=sent, recv_sem=got, device_id=where, device_id_type=MESH).start()

    def send(target, j, sem):
        push(planes.at[target, j], part(ma, pol, j), z_send, sem, {"ma": target})

    def send_last(i, target, j):
        send(target, j, z_last.at[j])
        if j == splits - 1 and {i, target} == {low - 1, low}:
            @pl.when(pol == 0)
            def _():
                push(planes.at[target, j], part(ma, pol, j), d_send, p_last.at[j], {"ma": target, "pol": 1})

    def whole(source, core):
        start = lax.rem(source, per_group) * per_source + core * block
        return recv.at[source // per_group, :, :, pl.ds(pl.multiple_of(start, block), block)]

    def await_all(ref, sem):
        pltpu.make_async_copy(ref, ref, sem).wait()

    def relay(source, j, sent, got, src=None):
        for q in range(1, n_pol):
            push(part(source, pol, j) if src is None else src, part(source, pol, j), sent, got,
                 {"pol": lax.rem(pol + q, n_pol)})

    def relayed(source):
        for q in range(1, n_pol):
            await_all(whole(source, lax.rem(pol + q, n_pol)), p_far.at[source])

    def send_phase(phase):
        for i in range(n_ma):
            near = i + 1 if i < low else i - 1
            outer = range(0, i) if i < low else range(i + 1, n_ma)
            plan = [(t, j) for t in far_first(n_ma, i) for j in range(splits)]
            first = [(near, j) for j in range(width)]
            second = [(t, j) for t, j in plan if t in outer]
            now = (first, second, [step for step in plan if step not in first + second])[phase]
            if now:
                @pl.when(ma == i)
                def _():
                    for t, j in now:
                        if i == across(n_ma, t):
                            send_last(i, t, j)
                        else:
                            send(t, j, z_far.at[i])

    turn(0)
    if few:
        send_phase(0)
    for h in range(1, pieces):
        turn(h)
    noise_copy.start()
    beam_copy.start()

    with mark("edge0"):
        @pl.when(has_outward)
        def _():
            pl.semaphore_wait(edge.at[0], 1)

    @pl.when(is_hub)
    def _():
        tell_line(inward, edge.at[1])

    @pl.when(jnp.logical_and(has_outward, jnp.logical_not(is_hub)))
    def _():
        tell_line(inward, edge.at[0])

    if few:
        send_phase(1)
    with mark("edge1"):
        pl.semaphore_wait(edge.at[1], 1)

    @pl.when(has_outward)
    def _():
        tell_line(outward, edge.at[1])

    if few:
        send_phase(2)
    else:
        for j in range(splits):
            loop(1, n_ma, lambda q: send(lax.rem(ma + q, n_ma), j, z_far.at[ma]))

    for j in range(splits):
        relay(ma, j, p_send.at[0], p_far.at[ma], planes.at[ma, j])
        for c in range(2):
            part(ma, pol, j)[c] = planes[ma, j, c]

    noise_copy.wait()
    spread = jnp.transpose(jnp.broadcast_to(noise_ref[...], (LANES, modes)))
    inv_n[...] = 1.0 / spread
    rs_n[...] = lax.rsqrt(spread)
    mine[1:2, :] = jnp.full((1, LANES), mask_ref[0].astype(jnp.float32))
    beam_copy.wait()
    strip = min(modes, 128)

    def widen(i):
        k0 = pl.multiple_of(i * strip, strip)
        for g in range(groups):
            degree = lax.broadcasted_iota(jnp.int32, (strip, rows), 1) + g * rows
            keep = degree >= m_ref[0]
            zero = jnp.zeros((strip, rows), jnp.float32)
            b0 = jnp.where(keep, beam_v[0, pl.ds(k0, strip), g * rows:(g + 1) * rows].astype(jnp.float32), zero)
            b1 = jnp.where(keep, beam_v[1, pl.ds(k0, strip), g * rows:(g + 1) * rows].astype(jnp.float32), zero)
            wide[g, pl.ds(k0, strip), 0:rows] = b0.astype(wide.dtype)
            wide[g, pl.ds(k0, strip), rows:2 * rows] = (-b1).astype(wide.dtype)
            wide[g, pl.ds(modes + k0, strip), 0:rows] = b1.astype(wide.dtype)
            wide[g, pl.ds(modes + k0, strip), rows:2 * rows] = b0.astype(wide.dtype)

    with mark("widen"):
        loop(0, modes // strip, widen)
    tell("pol", pol, n_pol, meet.at[0])
    pl.semaphore_wait(meet.at[0], n_pol - 1)
    tell("freq", freq, n_freq, meet.at[1])
    pl.semaphore_wait(meet.at[1], n_freq - 1)

    tile = min(modes, 256)

    def add(g, first=False):
        x = jnp.concatenate([recv[g, j].reshape(2 * rows, lanes) for j in range(splits)], axis=1)

        def body(k0):
            value = jnp.dot(wide[g, pl.ds(k0, tile), :], x, preferred_element_type=jnp.float32)
            acc[pl.ds(k0, tile), :] = value if first else acc[pl.ds(k0, tile), :] + value

        for i in range(2 * modes // tile):
            body(i * tile)

    def half(g, j, core):
        start = pl.multiple_of(core * block, block)
        x = jnp.concatenate([recv[g, j, c, pl.ds(start, block), :] for c in range(2)], axis=0)

        def value(k0):
            left = jnp.concatenate([wide[g, k0:k0 + tile, pl.ds(pl.multiple_of(c * rows + start, block), block)]
                                    for c in range(2)], axis=1)
            return jnp.dot(left, x, preferred_element_type=jnp.float32)
        return value

    def add_to(j, product):
        for i in range(2 * modes // tile):
            acc[i * tile:(i + 1) * tile, j * lanes:(j + 1) * lanes] += product(i * tile)

    def finish(g, j, power, product=None):
        for i in range(2 * modes // tile):
            at = (slice(i * tile, (i + 1) * tile), slice(j * lanes, (j + 1) * lanes))
            value = acc[at]
            if product is not None:
                value = value + product(i * tile)
                acc[at] = value
            k0 = i * tile % modes
            weighted = value * value * inv_n[k0:k0 + tile, :]
            power = power + jnp.sum(weighted.reshape(tile // 8, 8, lanes), axis=0)
        return power

    power = jnp.zeros((8, lanes), jnp.float32)
    if few:
        order = [pick_by(ma, [processing_order(n_ma, i)[k] for i in range(n_ma)]) for k in range(n_ma - 1)]
        last, before = order[-1], ma

        def settle(source, first):
            with mark("relay"):
                relayed(source)
            with mark("add"):
                add(source, first)

        for k in range(n_ma - 2):
            with mark(f"wait{k}"):
                await_all(whole(order[k], pol), z_far.at[order[k]])
            for j in range(splits):
                relay(order[k], j, p_send.at[1], p_far.at[order[k]])
            settle(before, k == 0)
            before = order[k]
        end = splits - 1
        direct = jnp.logical_and(is_hub, pol == 0)
        for j in range(splits):
            with mark(f"last{j}"):
                await_all(part(last, pol, j), z_last.at[j])
            if j < end:
                relay(last, j, p_send.at[2], p_last.at[j])
            else:
                @pl.when(jnp.logical_not(direct))
                def _():
                    relay(last, end, d_send, p_last.at[end])
            if j == 0:
                settle(before, n_ma == 2)
            add_to(j, half(last, j, pol))
            if j > 0:
                with mark(f"hop{j - 1}"):
                    await_all(part(last, 1 - pol, j - 1), p_last.at[j - 1])
                power = finish(last, j - 1, power, half(last, j - 1, 1 - pol))
        with mark("hoplast"):
            await_all(part(last, 1 - pol, end), p_last.at[end])
        power = finish(last, end, power, half(last, end, 1 - pol))
    else:
        def pass_on(source):
            @pl.when(source != ma)
            def _():
                await_all(whole(source, pol), z_far.at[source])
                for j in range(splits):
                    relay(source, j, p_send.at[1], p_far.at[source])
        loop(0, n_ma, pass_on)
        loop(0, n_ma, relayed)
        for g in range(groups):
            add(g, g == 0)
        for j in range(splits):
            power = finish(None, j, power)

    row = jnp.sum(power, axis=0, keepdims=True)
    mine[0:1, :] = row
    slots[my_slot, 0:1, :] = row
    slots[my_slot, 1:2, :] = mine[1:2, :]

    def report(r):
        pltpu.make_async_remote_copy(
            src_ref=mine, dst_ref=slots.at[my_slot], send_sem=q_send, recv_sem=q_recv,
            device_id=place(lax.rem(my_slot + r, n_all)), device_id_type=MESH).start()

    for_peers(report)

    with mark("drain"):
        await_all(planes.at[pl.ds(0, n_ma - 1)], z_send)
        await_all(planes.at[0], p_send.at[0])
        if few:
            if n_ma > 2:
                await_all(planes.at[pl.ds(0, n_ma - 2)], p_send.at[1])
            await_all(planes.at[0, pl.ds(0, splits - 1)], p_send.at[2])
            await_all(planes.at[0, 0], d_send)
        else:
            await_all(planes.at[pl.ds(0, n_ma - 1)], p_send.at[1])
    with mark("heard"):
        await_all(slots.at[pl.ds(0, n_all - 1)], q_recv)

    per_freq = n_ma * n_pol
    tail = mark('tail'); tail.__enter__()
    masked, live, here = 0.0, 0.0, 0.0
    for f in range(n_freq):
        channel = jnp.sum(jnp.sum(slots[f * per_freq:(f + 1) * per_freq, 0, :], axis=0, keepdims=True), axis=1, keepdims=True) / total
        flag = slots[f * per_freq, 1:2, 0:1]
        masked += flag * channel
        live += flag
        here += jnp.where(freq == f, channel, 0.0)
    band = masked / live
    factor = mine[1:2, 0:1] / jnp.sqrt(0.5 * here + 0.5 * band + 1e-06)
    power_ref[...] = jnp.broadcast_to(here, power_ref.shape)
    scale_ref[...] = rs_n[...] * factor
    await_all(slots.at[pl.ds(0, n_all - 1)], q_send)
    tail.__exit__(None,None,None)


def rescale_kernel(acc, scale_ref, power_ref, out_ref, channel_ref, staged, channel, sems, channel_sem):
    modes = scale_ref.shape[0]
    columns = acc.shape[1]
    strip = modes // sems.shape[0]
    channel[0] = power_ref[0, 0]
    last = pltpu.make_async_copy(channel, channel_ref, channel_sem)
    copies = []
    for i in range(sems.shape[0]):
        k0 = i * strip
        scale = scale_ref[k0:k0 + strip, :]
        for c in range(2):
            for j in range(columns // LANES):
                value = acc[c * modes + k0:c * modes + k0 + strip, j * LANES:(j + 1) * LANES]
                staged[c, k0:k0 + strip, j * LANES:(j + 1) * LANES] = (value * scale).astype(staged.dtype)
        copies.append(pltpu.make_async_copy(
            staged.at[:, pl.ds(k0, strip)], out_ref.at[:, pl.ds(k0, strip)], sems.at[i]))
        copies[-1].start()
        if i == 0:
            last.start()
    for copy in copies:
        copy.wait()
    last.wait()


def on_device(sizes, alm, beam, m_table, chan_mask, noise):
    n_ma, n_freq, n_pol = sizes
    coeffs = alm[:, 0]
    response = beam[0, 0]
    block, columns = coeffs.shape[1], coeffs.shape[3]
    modes, degrees = response.shape[1], response.shape[2]
    per_source = n_pol * block
    rows = per_source * max(1, min(n_ma, 256 // per_source))
    groups = degrees // rows
    splits = columns // LANES
    n_all = n_ma * n_freq * n_pol
    total = float(n_ma * modes * n_pol * columns)
    vmem = pl.BlockSpec(memory_space=pltpu.VMEM)
    hbm = pl.BlockSpec(memory_space=pltpu.HBM)
    smem = pl.BlockSpec(memory_space=pltpu.SMEM)
    dma = pltpu.SemaphoreType.DMA
    keep = functools.partial(pltpu.with_memory_space_constraint, memory_space=pltpu.HBM)
    visibility, scale, power = pl.pallas_call(
        functools.partial(step_kernel, sizes, total),
        out_shape=(
            jax.ShapeDtypeStruct((2 * modes, columns), jnp.float32),
            jax.ShapeDtypeStruct((modes, LANES), jnp.float32),
            jax.ShapeDtypeStruct((1, LANES), jnp.float32),
        ),
        in_specs=[hbm, hbm, smem, smem, hbm],
        out_specs=(vmem, vmem, vmem),
        scratch_shapes=[
            pltpu.VMEM((2, block, n_ma, columns), jnp.bfloat16),
            pltpu.VMEM((n_ma, splits, 2, block, LANES), jnp.bfloat16),
            pltpu.VMEM((groups, splits, 2, rows, LANES), jnp.bfloat16),
            pltpu.VMEM((groups, 2 * modes, 2 * rows), jnp.bfloat16),
            pltpu.VMEM((2, modes, degrees), jnp.bfloat16),
            pltpu.VMEM((modes, LANES), jnp.float32),
            pltpu.VMEM((modes, LANES), jnp.float32),
            pltpu.VMEM((2, LANES), jnp.float32),
            pltpu.VMEM((n_all, 2, LANES), jnp.float32),
            pltpu.VMEM((1, modes), jnp.float32),
            dma, dma((n_ma,)), dma((splits,)), dma, dma((3,)), dma((n_ma,)), dma((splits,)),
            dma((2 if splits % 2 == 0 else 1,)), dma, dma, dma,
            pltpu.SemaphoreType.REGULAR((2,)), pltpu.SemaphoreType.REGULAR((2,)), dma,
        ],
        compiler_params=pltpu.CompilerParams(collective_id=0, has_side_effects=True, vmem_limit_bytes=40 * 1024 * 1024),
        name="driftscan_step",
    )(keep(coeffs), keep(response), m_table, chan_mask, keep(noise))
    pieces = 8 if modes % 128 == 0 else 1
    scaled, channel_power = pl.pallas_call(
        rescale_kernel,
        out_shape=(
            jax.ShapeDtypeStruct((2, modes, columns), jnp.bfloat16),
            jax.ShapeDtypeStruct((1,), jnp.float32),
        ),
        in_specs=[vmem, vmem, vmem],
        out_specs=(hbm, hbm),
        scratch_shapes=[pltpu.VMEM((2, modes, columns), jnp.bfloat16), pltpu.SMEM((1,), jnp.float32), dma((pieces,)), dma],
        compiler_params=pltpu.CompilerParams(vmem_limit_bytes=16 * 1024 * 1024),
        name="rescale",
    )(visibility, scale, power)
    return scaled[:, None, None], channel_power


def solution(mesh):
    sizes = (mesh.shape["ma"], mesh.shape["freq"], mesh.shape["pol"])
    return jax.shard_map(
        functools.partial(on_device, sizes),
        mesh=mesh,
        in_specs=(
            P(None, "freq", ("ma", "pol"), None, "sky"),
            P("ma", "freq", None, "pol", None),
            P("ma"),
            P("freq"),
            P("freq", "pol"),
        ),
        out_specs=(P(None, "freq", "ma", "pol", "sky"), P(("sky", "freq"))),
        check_vma=False,
    )
```

```python
import contextlib
import functools

import jax
import jax.numpy as jnp
from jax import lax
from jax.experimental import pallas as pl
from jax.experimental.pallas import tpu as pltpu
from jax.sharding import PartitionSpec as P

MESH = pl.DeviceIdType.MESH
LANES = 128


def mark(name):
    return contextlib.nullcontext()


def across(n, i):
    return n // 2 if 2 * i < n else n // 2 - 1


def processing_order(n, i):
    last = across(n, i)
    rest = sorted((j for j in range(n) if j not in (i, last)), key=lambda j: (-abs(j - i), j))
    return rest + ([last] if last != i else [])


def far_first(n, i):
    return sorted((j for j in range(n) if j != i), key=lambda j: (-abs(j - i), j != across(n, i), j))


def pick_by(me, values):
    pick = jnp.int32(values[0])
    for i in range(1, len(values)):
        pick = jnp.where(me == i, jnp.int32(values[i]), pick)
    return pick


def step_kernel(
    sizes, total, alm_hbm, beam_hbm, m_ref, mask_ref, noise_hbm, acc, scale_ref, power_ref,
    staged, planes, recv, wide, beam_v, inv_n, rs_n, mine, slots, total_ref, noise_ref,
    z_send, z_far, z_last, d_send, p_send, p_far, p_last, in_sem, beam_sem, q_send, q_recv, edge, meet, small_sem,
):
    n_ma, n_freq, n_pol = sizes
    n_all = n_ma * n_freq * n_pol
    ma, freq, pol = lax.axis_index("ma"), lax.axis_index("freq"), lax.axis_index("pol")
    block = staged.shape[1]
    groups, splits, _, rows, lanes = recv.shape
    per_source = n_pol * block
    per_group = rows // per_source
    modes = beam_hbm.shape[1]
    my_slot = (freq * n_ma + ma) * n_pol + pol
    few = n_ma <= 8 and per_group == 1 and n_pol == 2 and block % LANES == 0 and splits > 1

    def place(slot):
        return {"ma": lax.rem(slot // n_pol, n_ma), "freq": slot // (n_pol * n_ma), "pol": lax.rem(slot, n_pol)}

    def loop(low, high, body, unroll=False):
        if unroll:
            for r in range(low, high):
                body(r)
        else:
            lax.fori_loop(low, high, lambda r, _: (body(r), 0)[1], 0)

    def for_peers(body):
        loop(1, n_all, body, n_all <= 32)

    barrier = pltpu.get_barrier_semaphore()

    def tell(axis, me, n, sem):
        loop(1, n, lambda q: pl.semaphore_signal(
            sem, inc=1, device_id={axis: lax.rem(me + q, n)}, device_id_type=MESH), n <= 8)

    low = n_ma // 2
    below = ma < low
    inward, outward = jnp.where(below, ma + 1, ma - 1), jnp.where(below, ma - 1, ma + 1)
    is_hub = jnp.logical_or(ma == low - 1, ma == low)
    has_outward = jnp.logical_and(ma > 0, ma < n_ma - 1)

    def tell_line(there, sem):
        pl.semaphore_signal(sem, inc=1, device_id={"ma": there}, device_id_type=MESH)

    @pl.when(is_hub)
    def _():
        tell_line(inward, barrier)

    @pl.when(has_outward)
    def _():
        tell_line(outward, barrier)

    tell("pol", pol, n_pol, barrier)
    tell("freq", freq, n_freq, barrier)

    def columns_of(j):
        return pl.ds(j * lanes, lanes)

    loads = [pltpu.make_async_copy(alm_hbm.at[:, :, :, columns_of(j)], staged.at[:, :, :, columns_of(j)], in_sem.at[j])
             for j in range(splits)]
    for load in loads:
        load.start()
    noise_copy = pltpu.make_async_copy(noise_hbm, noise_ref, small_sem)
    beam_copy = pltpu.make_async_copy(beam_hbm, beam_v, beam_sem)

    def part(source, core, j):
        start = lax.rem(source, per_group) * per_source + core * block
        return recv.at[source // per_group, j, :, pl.ds(pl.multiple_of(start, block), block)]

    is_end = jnp.logical_not(jnp.logical_or(is_hub, has_outward))

    def enter():
        pl.semaphore_wait(barrier, 1 + n_pol - 1 + n_freq - 1)

    @pl.when(is_end)
    def _():
        enter()
        tell_line(inward, edge.at[0])

    step = min(block, 16)

    def turn(j):
        with mark("load"):
            loads[j].wait()
        for c in range(2):
            for e in range(0, block, step):
                planes[:, j, c, e:e + step, :] = jnp.transpose(staged[c, e:e + step, :, columns_of(j)], (1, 0, 2))

    turn(0)
    with mark("barrier"):
        @pl.when(jnp.logical_not(is_end))
        def _():
            enter()

    def push(src, dst, sent, got, where):
        pltpu.make_async_remote_copy(
            src_ref=src, dst_ref=dst, send_sem=sent, recv_sem=got, device_id=where, device_id_type=MESH).start()

    def send(target, j, sem):
        push(planes.at[target, j], part(ma, pol, j), z_send, sem, {"ma": target})

    def send_last(i, target, j):
        send(target, j, z_last.at[j])
        if j == splits - 1 and {i, target} == {low - 1, low}:
            @pl.when(pol == 0)
            def _():
                push(planes.at[target, j], part(ma, pol, j), d_send, p_last.at[j], {"ma": target, "pol": 1})

    def whole(source, core):
        start = lax.rem(source, per_group) * per_source + core * block
        return recv.at[source // per_group, :, :, pl.ds(pl.multiple_of(start, block), block)]

    def await_all(ref, sem):
        pltpu.make_async_copy(ref, ref, sem).wait()

    def relay(source, j, sent, got, src=None):
        for q in range(1, n_pol):
            push(part(source, pol, j) if src is None else src, part(source, pol, j), sent, got,
                 {"pol": lax.rem(pol + q, n_pol)})

    def relayed(source):
        for q in range(1, n_pol):
            await_all(whole(source, lax.rem(pol + q, n_pol)), p_far.at[source])

    def send_phase(phase):
        for i in range(n_ma):
            near = i + 1 if i < low else i - 1
            outer = range(0, i) if i < low else range(i + 1, n_ma)
            plan = [(t, j) for t in far_first(n_ma, i) for j in range(splits)]
            first = [(near, j) for j in range(min(2, splits))]
            second = [(t, j) for t, j in plan if t in outer]
            rest = [step for step in plan if step not in first + second]
            now = (first[:1], first[1:], second, rest)[phase]
            if now:
                @pl.when(ma == i)
                def _():
                    for t, j in now:
                        if i == across(n_ma, t):
                            send_last(i, t, j)
                        else:
                            send(t, j, z_far.at[i])

    if few:
        send_phase(0)
    for j in range(1, splits):
        turn(j)
        if few and j == 1:
            send_phase(1)
    noise_copy.start()
    beam_copy.start()

    with mark("edge0"):
        @pl.when(has_outward)
        def _():
            pl.semaphore_wait(edge.at[0], 1)

    @pl.when(is_hub)
    def _():
        tell_line(inward, edge.at[1])

    @pl.when(jnp.logical_and(has_outward, jnp.logical_not(is_hub)))
    def _():
        tell_line(inward, edge.at[0])

    if few:
        send_phase(2)
    with mark("edge1"):
        pl.semaphore_wait(edge.at[1], 1)

    @pl.when(has_outward)
    def _():
        tell_line(outward, edge.at[1])

    if few:
        send_phase(3)
    else:
        for j in range(splits):
            loop(1, n_ma, lambda q: send(lax.rem(ma + q, n_ma), j, z_far.at[ma]))

    for j in range(splits):
        relay(ma, j, p_send.at[0], p_far.at[ma], planes.at[ma, j])
        for c in range(2):
            part(ma, pol, j)[c] = planes[ma, j, c]

    noise_copy.wait()
    spread = jnp.transpose(jnp.broadcast_to(noise_ref[...], (LANES, modes)))
    inv_n[...] = 1.0 / spread
    rs_n[...] = lax.rsqrt(spread)
    mine[1:2, :] = jnp.full((1, LANES), mask_ref[0].astype(jnp.float32))
    beam_copy.wait()
    strip = min(modes, 128)

    def widen(i):
        k0 = pl.multiple_of(i * strip, strip)
        for g in range(groups):
            degree = lax.broadcasted_iota(jnp.int32, (strip, rows), 1) + g * rows
            keep = degree >= m_ref[0]
            zero = jnp.zeros((strip, rows), jnp.float32)
            b0 = jnp.where(keep, beam_v[0, pl.ds(k0, strip), g * rows:(g + 1) * rows].astype(jnp.float32), zero)
            b1 = jnp.where(keep, beam_v[1, pl.ds(k0, strip), g * rows:(g + 1) * rows].astype(jnp.float32), zero)
            wide[g, pl.ds(k0, strip), 0:rows] = b0.astype(wide.dtype)
            wide[g, pl.ds(k0, strip), rows:2 * rows] = (-b1).astype(wide.dtype)
            wide[g, pl.ds(modes + k0, strip), 0:rows] = b1.astype(wide.dtype)
            wide[g, pl.ds(modes + k0, strip), rows:2 * rows] = b0.astype(wide.dtype)

    with mark("widen"):
        loop(0, modes // strip, widen)
    tell("pol", pol, n_pol, meet.at[0])
    pl.semaphore_wait(meet.at[0], n_pol - 1)
    tell("freq", freq, n_freq, meet.at[1])
    pl.semaphore_wait(meet.at[1], n_freq - 1)

    tile = min(modes, 256)

    def add(g, first=False):
        x = jnp.concatenate([recv[g, j].reshape(2 * rows, lanes) for j in range(splits)], axis=1)

        def body(k0):
            value = jnp.dot(wide[g, pl.ds(k0, tile), :], x, preferred_element_type=jnp.float32)
            acc[pl.ds(k0, tile), :] = value if first else acc[pl.ds(k0, tile), :] + value

        for i in range(2 * modes // tile):
            body(i * tile)

    def half(g, first, end, core):
        start = pl.multiple_of(core * block, block)
        x = jnp.concatenate([jnp.concatenate([recv[g, j, c, pl.ds(start, block), :] for c in range(2)], axis=0)
                             for j in range(first, end)], axis=1)

        def value(k0):
            left = jnp.concatenate([wide[g, k0:k0 + tile, pl.ds(pl.multiple_of(c * rows + start, block), block)]
                                    for c in range(2)], axis=1)
            return jnp.dot(left, x, preferred_element_type=jnp.float32)
        return value

    def add_to(j, product):
        for i in range(2 * modes // tile):
            acc[i * tile:(i + 1) * tile, j * lanes:(j + 1) * lanes] += product(i * tile)

    def full(g, j):
        x = recv[g, j].reshape(2 * rows, lanes)
        return lambda k0: jnp.dot(wide[g, k0:k0 + tile, :], x, preferred_element_type=jnp.float32)

    def finish(first, end, product=None):
        power = total_ref[...]
        for i in range(2 * modes // tile):
            at = (slice(i * tile, (i + 1) * tile), slice(first * lanes, end * lanes))
            value = acc[at]
            if product is not None:
                value = value + product(i * tile)
                acc[at] = value
            k0 = i * tile % modes
            weights = inv_n[k0:k0 + tile, :]
            for j in range(end - first):
                one = value[:, j * lanes:(j + 1) * lanes]
                power = power + jnp.sum((one * one * weights).reshape(tile // 8, 8, lanes), axis=0)
        total_ref[...] = power

    total_ref[...] = jnp.zeros_like(total_ref)
    if few:
        order = [pick_by(ma, [processing_order(n_ma, i)[k] for i in range(n_ma)]) for k in range(n_ma - 1)]
        last, before = order[-1], ma

        def settle(source, first):
            with mark("relay"):
                relayed(source)
            with mark("add"):
                add(source, first)

        for k in range(n_ma - 2):
            with mark(f"wait{k}"):
                await_all(whole(order[k], pol), z_far.at[order[k]])
            for j in range(splits):
                relay(order[k], j, p_send.at[1], p_far.at[order[k]])
            settle(before, k == 0)
            before = order[k]
        end = splits - 1
        direct = jnp.logical_and(is_hub, pol == 0)

        def own_block(j):
            with mark(f"last{j}"):
                await_all(part(last, pol, j), z_last.at[j])

        def other_block(j):
            with mark(f"hop{j}"):
                await_all(part(last, 1 - pol, j), p_last.at[j])

        own_block(0)
        relay(last, 0, p_send.at[2], p_last.at[0])
        settle(before, n_ma == 2)

        @pl.when(direct)
        def _():
            for j in range(splits):
                if j > 0:
                    own_block(j)
                    if j < end:
                        relay(last, j, p_send.at[2], p_last.at[j])
                other_block(j)
                finish(j, j + 1, full(last, j))

        @pl.when(jnp.logical_not(direct))
        def _():
            for j in range(splits):
                if j > 0:
                    own_block(j)
                    relay(last, j, p_send.at[2] if j < end else d_send, p_last.at[j])
                add_to(j, half(last, j, j + 1, pol))
                if 0 < j < end:
                    other_block(j - 1)
                    finish(j - 1, j, half(last, j - 1, j, 1 - pol))
            other_block(end - 1)
            other_block(end)
            finish(end - 1, splits, half(last, end - 1, splits, 1 - pol))
    else:
        def pass_on(source):
            @pl.when(source != ma)
            def _():
                await_all(whole(source, pol), z_far.at[source])
                for j in range(splits):
                    relay(source, j, p_send.at[1], p_far.at[source])
        loop(0, n_ma, pass_on)
        loop(0, n_ma, relayed)
        for g in range(groups):
            add(g, g == 0)
        for j in range(splits):
            finish(j, j + 1)

    row = jnp.sum(total_ref[...], axis=0, keepdims=True)
    mine[0:1, :] = row
    slots[my_slot, 0:1, :] = row
    slots[my_slot, 1:2, :] = mine[1:2, :]

    def report(r):
        pltpu.make_async_remote_copy(
            src_ref=mine, dst_ref=slots.at[my_slot], send_sem=q_send, recv_sem=q_recv,
            device_id=place(lax.rem(my_slot + r, n_all)), device_id_type=MESH).start()

    for_peers(report)

    with mark("drain"):
        await_all(planes.at[pl.ds(0, n_ma - 1)], z_send)
        await_all(planes.at[0], p_send.at[0])
        if few:
            if n_ma > 2:
                await_all(planes.at[pl.ds(0, n_ma - 2)], p_send.at[1])
            await_all(planes.at[0, pl.ds(0, splits - 1)], p_send.at[2])
            await_all(planes.at[0, 0], d_send)
        else:
            await_all(planes.at[pl.ds(0, n_ma - 1)], p_send.at[1])
    with mark("heard"):
        await_all(slots.at[pl.ds(0, n_all - 1)], q_recv)

    per_freq = n_ma * n_pol
    tail = mark('tail'); tail.__enter__()
    masked, live, here = 0.0, 0.0, 0.0
    for f in range(n_freq):
        channel = jnp.sum(jnp.sum(slots[f * per_freq:(f + 1) * per_freq, 0, :], axis=0, keepdims=True), axis=1, keepdims=True) / total
        flag = slots[f * per_freq, 1:2, 0:1]
        masked += flag * channel
        live += flag
        here += jnp.where(freq == f, channel, 0.0)
    band = masked / live
    factor = mine[1:2, 0:1] / jnp.sqrt(0.5 * here + 0.5 * band + 1e-06)
    power_ref[...] = jnp.broadcast_to(here, power_ref.shape)
    scale_ref[...] = rs_n[...] * factor
    await_all(slots.at[pl.ds(0, n_all - 1)], q_send)
    tail.__exit__(None,None,None)


def rescale_kernel(acc, scale_ref, power_ref, out_ref, channel_ref, staged, channel, sems, channel_sem):
    modes = scale_ref.shape[0]
    columns = acc.shape[1]
    strip = modes // sems.shape[0]
    channel[0] = power_ref[0, 0]
    last = pltpu.make_async_copy(channel, channel_ref, channel_sem)
    copies = []
    for i in range(sems.shape[0]):
        k0 = i * strip
        scale = scale_ref[k0:k0 + strip, :]
        for c in range(2):
            for j in range(columns // LANES):
                value = acc[c * modes + k0:c * modes + k0 + strip, j * LANES:(j + 1) * LANES]
                staged[c, k0:k0 + strip, j * LANES:(j + 1) * LANES] = (value * scale).astype(staged.dtype)
        copies.append(pltpu.make_async_copy(
            staged.at[:, pl.ds(k0, strip)], out_ref.at[:, pl.ds(k0, strip)], sems.at[i]))
        copies[-1].start()
        if i == 0:
            last.start()
    for copy in copies:
        copy.wait()
    last.wait()


def on_device(sizes, alm, beam, m_table, chan_mask, noise):
    n_ma, n_freq, n_pol = sizes
    coeffs = alm[:, 0]
    response = beam[0, 0]
    block, columns = coeffs.shape[1], coeffs.shape[3]
    modes, degrees = response.shape[1], response.shape[2]
    per_source = n_pol * block
    rows = per_source * max(1, min(n_ma, 256 // per_source))
    groups = degrees // rows
    splits = columns // LANES
    n_all = n_ma * n_freq * n_pol
    total = float(n_ma * modes * n_pol * columns)
    vmem = pl.BlockSpec(memory_space=pltpu.VMEM)
    hbm = pl.BlockSpec(memory_space=pltpu.HBM)
    smem = pl.BlockSpec(memory_space=pltpu.SMEM)
    dma = pltpu.SemaphoreType.DMA
    keep = functools.partial(pltpu.with_memory_space_constraint, memory_space=pltpu.HBM)
    visibility, scale, power = pl.pallas_call(
        functools.partial(step_kernel, sizes, total),
        out_shape=(
            jax.ShapeDtypeStruct((2 * modes, columns), jnp.float32),
            jax.ShapeDtypeStruct((modes, LANES), jnp.float32),
            jax.ShapeDtypeStruct((1, LANES), jnp.float32),
        ),
        in_specs=[hbm, hbm, smem, smem, hbm],
        out_specs=(vmem, vmem, vmem),
        scratch_shapes=[
            pltpu.VMEM((2, block, n_ma, columns), jnp.bfloat16),
            pltpu.VMEM((n_ma, splits, 2, block, LANES), jnp.bfloat16),
            pltpu.VMEM((groups, splits, 2, rows, LANES), jnp.bfloat16),
            pltpu.VMEM((groups, 2 * modes, 2 * rows), jnp.bfloat16),
            pltpu.VMEM((2, modes, degrees), jnp.bfloat16),
            pltpu.VMEM((modes, LANES), jnp.float32),
            pltpu.VMEM((modes, LANES), jnp.float32),
            pltpu.VMEM((2, LANES), jnp.float32),
            pltpu.VMEM((n_all, 2, LANES), jnp.float32),
            pltpu.VMEM((8, LANES), jnp.float32),
            pltpu.VMEM((1, modes), jnp.float32),
            dma, dma((n_ma,)), dma((splits,)), dma, dma((3,)), dma((n_ma,)), dma((splits,)),
            dma((splits,)), dma, dma, dma,
            pltpu.SemaphoreType.REGULAR((2,)), pltpu.SemaphoreType.REGULAR((2,)), dma,
        ],
        compiler_params=pltpu.CompilerParams(collective_id=0, has_side_effects=True, vmem_limit_bytes=40 * 1024 * 1024),
        name="driftscan_step",
    )(keep(coeffs), keep(response), m_table, chan_mask, keep(noise))
    pieces = 8 if modes % 128 == 0 else 1
    scaled, channel_power = pl.pallas_call(
        rescale_kernel,
        out_shape=(
            jax.ShapeDtypeStruct((2, modes, columns), jnp.bfloat16),
            jax.ShapeDtypeStruct((1,), jnp.float32),
        ),
        in_specs=[vmem, vmem, vmem],
        out_specs=(hbm, hbm),
        scratch_shapes=[pltpu.VMEM((2, modes, columns), jnp.bfloat16), pltpu.SMEM((1,), jnp.float32), dma((pieces,)), dma],
        compiler_params=pltpu.CompilerParams(vmem_limit_bytes=16 * 1024 * 1024),
        name="rescale",
    )(visibility, scale, power)
    return scaled[:, None, None], channel_power


def solution(mesh):
    sizes = (mesh.shape["ma"], mesh.shape["freq"], mesh.shape["pol"])
    return jax.shard_map(
        functools.partial(on_device, sizes),
        mesh=mesh,
        in_specs=(
            P(None, "freq", ("ma", "pol"), None, "sky"),
            P("ma", "freq", None, "pol", None),
            P("ma"),
            P("freq"),
            P("freq", "pol"),
        ),
        out_specs=(P(None, "freq", "ma", "pol", "sky"), P(("sky", "freq"))),
        check_vma=False,
    )
```

```python
import contextlib
import functools

import jax
import jax.numpy as jnp
from jax import lax
from jax.experimental import pallas as pl
from jax.experimental.pallas import tpu as pltpu
from jax.sharding import PartitionSpec as P

MESH = pl.DeviceIdType.MESH
LANES = 128


def mark(name):
    return contextlib.nullcontext()


def across(n, i):
    return n // 2 if 2 * i < n else n // 2 - 1


def processing_order(n, i):
    last = across(n, i)
    rest = sorted((j for j in range(n) if j not in (i, last)), key=lambda j: (-abs(j - i), j))
    return rest + ([last] if last != i else [])


def far_first(n, i):
    return sorted((j for j in range(n) if j != i), key=lambda j: (-abs(j - i), j != across(n, i), j))


def pick_by(me, values):
    pick = jnp.int32(values[0])
    for i in range(1, len(values)):
        pick = jnp.where(me == i, jnp.int32(values[i]), pick)
    return pick


def step_kernel(
    sizes, total, alm_hbm, beam_hbm, m_ref, mask_ref, noise_hbm, acc, scale_ref, power_ref,
    staged, planes, extra, recv, wide, wide_o, beam_v, beam_o, acc_o, incoming, inv_n, inv_o, rs_n, mine, slots, total_ref,
    noise_ref, noise_o,
    z_send, near_send, x_send, x_recv, b_send, b_recv, i_send, i_recv, z_far, z_last, y_last, p_send, p_far, p_last, in_sem, beam_sem, q_send, q_recv, edge, meet, small_sem,
):
    n_ma, n_freq, n_pol = sizes
    n_all = n_ma * n_freq * n_pol
    ma, freq, pol = lax.axis_index("ma"), lax.axis_index("freq"), lax.axis_index("pol")
    block = staged.shape[1]
    groups, splits, _, rows, lanes = recv.shape
    per_source = n_pol * block
    per_group = rows // per_source
    modes = beam_hbm.shape[1]
    my_slot = (freq * n_ma + ma) * n_pol + pol
    few = 2 < n_ma <= 8 and per_group == 1 and n_pol == 2 and block % LANES == 0 and splits > 3

    def place(slot):
        return {"ma": lax.rem(slot // n_pol, n_ma), "freq": slot // (n_pol * n_ma), "pol": lax.rem(slot, n_pol)}

    def loop(low, high, body, unroll=False):
        if unroll:
            for r in range(low, high):
                body(r)
        else:
            lax.fori_loop(low, high, lambda r, _: (body(r), 0)[1], 0)

    def for_peers(body):
        loop(1, n_all, body, n_all <= 32)

    barrier = pltpu.get_barrier_semaphore()

    def tell(axis, me, n, sem):
        loop(1, n, lambda q: pl.semaphore_signal(
            sem, inc=1, device_id={axis: lax.rem(me + q, n)}, device_id_type=MESH), n <= 8)

    low = n_ma // 2
    below = ma < low
    inward, outward = jnp.where(below, ma + 1, ma - 1), jnp.where(below, ma - 1, ma + 1)
    is_hub = jnp.logical_or(ma == low - 1, ma == low)
    has_outward = jnp.logical_and(ma > 0, ma < n_ma - 1)
    hub_lead, hub_other = jnp.logical_and(is_hub, pol == 1), jnp.logical_and(is_hub, pol == 0)

    def tell_line(there, sem):
        pl.semaphore_signal(sem, inc=1, device_id={"ma": there}, device_id_type=MESH)

    @pl.when(is_hub)
    def _():
        tell_line(inward, barrier)

    @pl.when(has_outward)
    def _():
        tell_line(outward, barrier)

    tell("pol", pol, n_pol, barrier)
    tell("freq", freq, n_freq, barrier)

    def columns_of(j):
        return pl.ds(j * lanes, lanes)

    loads = [pltpu.make_async_copy(alm_hbm.at[:, :, :, columns_of(j)], staged.at[:, :, :, columns_of(j)], in_sem.at[j])
             for j in range(splits)]
    for load in loads:
        load.start()
    noise_copy = pltpu.make_async_copy(noise_hbm, noise_ref, small_sem)
    beam_copy = pltpu.make_async_copy(beam_hbm, beam_v, beam_sem)

    def part(source, core, j):
        start = lax.rem(source, per_group) * per_source + core * block
        return recv.at[source // per_group, j, :, pl.ds(pl.multiple_of(start, block), block)]

    is_end = jnp.logical_not(jnp.logical_or(is_hub, has_outward))

    def enter():
        pl.semaphore_wait(barrier, 1 + n_pol - 1 + n_freq - 1)

    @pl.when(is_end)
    def _():
        enter()
        tell_line(inward, edge.at[0])

    step = min(block, 16)

    def turn(j):
        with mark("load"):
            loads[j].wait()
        for c in range(2):
            for e in range(0, block, step):
                planes[:, j, c, e:e + step, :] = jnp.transpose(staged[c, e:e + step, :, columns_of(j)], (1, 0, 2))

    turn(0)
    with mark("barrier"):
        @pl.when(jnp.logical_not(is_end))
        def _():
            enter()

    def push(src, dst, sent, got, where):
        pltpu.make_async_remote_copy(
            src_ref=src, dst_ref=dst, send_sem=sent, recv_sem=got, device_id=where, device_id_type=MESH).start()

    def send(target, j, got, sent):
        push(planes.at[target, j], part(ma, pol, j), sent, got, {"ma": target})

    def whole(source, core):
        start = lax.rem(source, per_group) * per_source + core * block
        return recv.at[source // per_group, :, :, pl.ds(pl.multiple_of(start, block), block)]

    def await_all(ref, sem):
        pltpu.make_async_copy(ref, ref, sem).wait()

    def relay(source, j, sent, got, src=None):
        for q in range(1, n_pol):
            push(part(source, pol, j) if src is None else src, part(source, pol, j), sent, got,
                 {"pol": lax.rem(pol + q, n_pol)})

    def relayed(source):
        for q in range(1, n_pol):
            await_all(whole(source, lax.rem(pol + q, n_pol)), p_far.at[source])

    held = splits - 2

    def send_phase(phase):
        for i in range(n_ma):
            near = i + 1 if i < low else i - 1
            outer = range(0, i) if i < low else range(i + 1, n_ma)
            plan = [(t, j) for t in far_first(n_ma, i) for j in range(splits)]
            first = [(near, j) for j in range(2)]
            second = [(t, j) for t, j in plan if t in outer]
            rest = [step for step in plan if step not in first + second]
            hub = i in (low - 1, low)
            now = (first[:1], first[1:], second, rest)[phase]
            late = [(t, j) for t, j in now if hub and t == near and j >= held]
            if now:
                @pl.when(ma == i)
                def _():
                    for t, j in now:
                        if (t, j) not in late:
                            send(t, j, z_last.at[j] if i == across(n_ma, t) else z_far.at[i],
                                 near_send if t == near else z_send)
                    if late:
                        @pl.when(pol == 0)
                        def _():
                            push(planes.at[near, pl.ds(held, 2)], extra, near_send, x_recv, {"pol": 1})

                        @pl.when(pol == 1)
                        def _():
                            await_all(extra, x_recv)
                            for t, j in late:
                                push(extra.at[j - held], part(ma, 0, j), x_send, y_last.at[j - held], {"ma": t})
                                send(t, j, z_last.at[j], near_send)

    if few:
        send_phase(0)
    for j in range(1, splits):
        turn(j)
        if few and j == 1:
            send_phase(1)
    noise_copy.start()
    beam_copy.start()

    with mark("edge0"):
        @pl.when(has_outward)
        def _():
            pl.semaphore_wait(edge.at[0], 1)

    @pl.when(is_hub)
    def _():
        tell_line(inward, edge.at[1])

    @pl.when(jnp.logical_and(has_outward, jnp.logical_not(is_hub)))
    def _():
        tell_line(inward, edge.at[0])

    if few:
        send_phase(2)
    with mark("edge1"):
        pl.semaphore_wait(edge.at[1], 1)

    @pl.when(has_outward)
    def _():
        tell_line(outward, edge.at[1])

    if few:
        send_phase(3)
    else:
        for j in range(splits):
            loop(1, n_ma, lambda q: send(lax.rem(ma + q, n_ma), j, z_far.at[ma], z_send))

    for j in range(splits):
        relay(ma, j, p_send.at[0], p_far.at[ma], planes.at[ma, j])
        for c in range(2):
            part(ma, pol, j)[c] = planes[ma, j, c]

    if few:
        @pl.when(hub_other)
        def _():
            push(beam_hbm, beam_o, b_send.at[0], b_recv.at[0], {"pol": 1})
            push(noise_hbm, noise_o, b_send.at[1], b_recv.at[1], {"pol": 1})

    noise_copy.wait()
    spread = jnp.transpose(jnp.broadcast_to(noise_ref[...], (LANES, modes)))
    inv_n[...] = 1.0 / spread
    rs_n[...] = lax.rsqrt(spread)
    mine[1:2, :] = jnp.full((1, LANES), mask_ref[0].astype(jnp.float32))
    beam_copy.wait()
    strip = min(modes, 128)

    def widen(beam_v, wide, i):
        k0 = pl.multiple_of(i * strip, strip)
        for g in range(groups):
            degree = lax.broadcasted_iota(jnp.int32, (strip, rows), 1) + g * rows
            keep = degree >= m_ref[0]
            zero = jnp.zeros((strip, rows), jnp.float32)
            b0 = jnp.where(keep, beam_v[0, pl.ds(k0, strip), g * rows:(g + 1) * rows].astype(jnp.float32), zero)
            b1 = jnp.where(keep, beam_v[1, pl.ds(k0, strip), g * rows:(g + 1) * rows].astype(jnp.float32), zero)
            wide[g, pl.ds(k0, strip), 0:rows] = b0.astype(wide.dtype)
            wide[g, pl.ds(k0, strip), rows:2 * rows] = (-b1).astype(wide.dtype)
            wide[g, pl.ds(modes + k0, strip), 0:rows] = b1.astype(wide.dtype)
            wide[g, pl.ds(modes + k0, strip), rows:2 * rows] = b0.astype(wide.dtype)

    with mark("widen"):
        loop(0, modes // strip, functools.partial(widen, beam_v, wide))
    tell("pol", pol, n_pol, meet.at[0])
    pl.semaphore_wait(meet.at[0], n_pol - 1)
    tell("freq", freq, n_freq, meet.at[1])
    pl.semaphore_wait(meet.at[1], n_freq - 1)

    if few:
        @pl.when(hub_lead)
        def _():
            await_all(noise_o, b_recv.at[1])
            inv_o[...] = 1.0 / jnp.transpose(jnp.broadcast_to(noise_o[...], (LANES, modes)))
            await_all(beam_o, b_recv.at[0])
            loop(0, modes // strip, functools.partial(widen, beam_o, wide_o))

    tile = min(modes, 256)

    def add(g, first=False):
        x = jnp.concatenate([recv[g, j].reshape(2 * rows, lanes) for j in range(splits)], axis=1)

        def body(k0):
            value = jnp.dot(wide[g, pl.ds(k0, tile), :], x, preferred_element_type=jnp.float32)
            acc[pl.ds(k0, tile), :] = value if first else acc[pl.ds(k0, tile), :] + value

        for i in range(2 * modes // tile):
            body(i * tile)

    def half(w, g, j, core):
        start = pl.multiple_of(core * block, block)
        x = jnp.concatenate([recv[g, j, c, pl.ds(start, block), :] for c in range(2)], axis=0)

        def value(k0):
            left = jnp.concatenate([w[g, k0:k0 + tile, pl.ds(pl.multiple_of(c * rows + start, block), block)]
                                    for c in range(2)], axis=1)
            return jnp.dot(left, x, preferred_element_type=jnp.float32)
        return value

    def full(w, g, j):
        x = recv[g, j].reshape(2 * rows, lanes)
        return lambda k0: jnp.dot(w[g, k0:k0 + tile, :], x, preferred_element_type=jnp.float32)

    def add_to(sums, j, product, first=False):
        for i in range(2 * modes // tile):
            at = (slice(i * tile, (i + 1) * tile), slice(j * lanes, (j + 1) * lanes))
            sums[at] = product(i * tile) if first else sums[at] + product(i * tile)

    def finish(sums, weights, j, product=None):
        power = total_ref[...]
        for i in range(2 * modes // tile):
            at = (slice(i * tile, (i + 1) * tile), slice(j * lanes, (j + 1) * lanes))
            value = sums[at]
            if product is not None:
                value = value + product(i * tile)
                sums[at] = value
            k0 = i * tile % modes
            weighted = value * value * weights[k0:k0 + tile, :]
            power = power + jnp.sum(weighted.reshape(tile // 8, 8, lanes), axis=0)
        total_ref[...] = power

    def finish_both(product, product_o):
        power, power_o = total_ref[...], jnp.zeros(total_ref.shape, jnp.float32)
        for i in range(2 * modes // tile):
            row, k0 = slice(i * tile, (i + 1) * tile), i * tile % modes
            value_o = acc_o[row, :] + product_o(i * tile)
            value = acc[row, (splits - 1) * lanes:] + product(i * tile)
            acc_o[row, :] = value_o
            acc[row, (splits - 1) * lanes:] = value
            power_o = power_o + jnp.sum((value_o * value_o * inv_o[k0:k0 + tile, :]).reshape(tile // 8, 8, lanes), axis=0)
            power = power + jnp.sum((value * value * inv_n[k0:k0 + tile, :]).reshape(tile // 8, 8, lanes), axis=0)
        total_ref[...] = power + power_o

    total_ref[...] = jnp.zeros_like(total_ref)
    if few:
        order = [pick_by(ma, [processing_order(n_ma, i)[k] for i in range(n_ma)]) for k in range(n_ma - 1)]
        last, end = order[-1], splits - 1

        def own_block(j):
            with mark(f"last{j}"):
                await_all(part(last, pol, j), z_last.at[j])

        def other_block(j):
            with mark(f"hop{j}"):
                await_all(part(last, 1 - pol, j), p_last.at[j])

        def pass_block(j, core=None, slot=None):
            at = part(last, pol if core is None else core, j)
            push(at, at, p_send.at[2], p_last.at[j if slot is None else slot], {"pol": 1 - pol})

        def take(k):
            with mark(f"wait{k}"):
                await_all(whole(order[k], pol), z_far.at[order[k]])
            for j in range(splits):
                relay(order[k], j, p_send.at[1], p_far.at[order[k]])

        def settle(source, first=False, shared=False):
            with mark("relay"):
                relayed(source)
            with mark("add"):
                add(source, first)
                if shared:
                    @pl.when(hub_lead)
                    def _():
                        add_to(acc_o, 0, full(wide_o, source, end), first)

        @pl.when(is_hub)
        def _():
            for j in range(held):
                own_block(j)
                pass_block(j)
            settle(ma, True, True)
            for j in range(held):
                other_block(j)
                add_to(acc, j, full(wide, last, j))
            for k in range(n_ma - 2):
                take(k)
                if k:
                    settle(order[k - 1], False, True)
            if n_ma > 2:
                settle(order[n_ma - 3], False, True)

        @pl.when(hub_lead)
        def _():
            with mark("y0"):
                await_all(part(last, 0, held), y_last.at[0])
            pass_block(held, 0, end)
            own_block(held)
            pass_block(held)
            for j in range(held):
                finish(acc, inv_n, j)
            finish(acc, inv_n, held, full(wide, last, held))
            with mark("y1"):
                await_all(part(last, 0, end), y_last.at[1])
            add_to(acc, end, half(wide, last, end, 0))
            add_to(acc_o, 0, half(wide_o, last, end, 0))
            own_block(end)
            finish_both(half(wide, last, end, 1), half(wide_o, last, end, 1))

        @pl.when(hub_other)
        def _():
            for j in range(held):
                finish(acc, inv_n, j)
            with mark("x"):
                await_all(part(last, 0, held), p_last.at[end])
            other_block(held)
            finish(acc, inv_n, held, full(wide, last, held))

        @pl.when(jnp.logical_not(is_hub))
        def _():
            before = ma
            for k in range(n_ma - 2):
                take(k)
                settle(before, k == 0)
                before = order[k]
            own_block(0)
            pass_block(0)
            settle(before)
            add_to(acc, 0, half(wide, last, 0, pol))
            for j in range(1, splits):
                own_block(j)
                pass_block(j)
                add_to(acc, j, half(wide, last, j, pol))
                other_block(j - 1)
                finish(acc, inv_n, j - 1, half(wide, last, j - 1, 1 - pol))
            other_block(end)
            finish(acc, inv_n, end, half(wide, last, end, 1 - pol))
    else:
        def pass_on(source):
            @pl.when(source != ma)
            def _():
                await_all(whole(source, pol), z_far.at[source])
                for j in range(splits):
                    relay(source, j, p_send.at[1], p_far.at[source])
        loop(0, n_ma, pass_on)
        loop(0, n_ma, relayed)
        for g in range(groups):
            add(g, g == 0)
        for j in range(splits):
            finish(acc, inv_n, j)

    row = jnp.sum(total_ref[...], axis=0, keepdims=True)
    mine[0:1, :] = row
    slots[my_slot, 0:1, :] = row
    slots[my_slot, 1:2, :] = mine[1:2, :]

    def report(r):
        pltpu.make_async_remote_copy(
            src_ref=mine, dst_ref=slots.at[my_slot], send_sem=q_send, recv_sem=q_recv,
            device_id=place(lax.rem(my_slot + r, n_all)), device_id_type=MESH).start()

    for_peers(report)
    if few:
        @pl.when(hub_lead)
        def _():
            push(acc_o, incoming, i_send, i_recv, {"pol": 0})

    with mark("drain"):
        await_all(planes.at[pl.ds(0, n_ma - 2 if few else n_ma - 1)], z_send)
        await_all(planes.at[0], p_send.at[0])
        if few:
            if n_ma > 2:
                await_all(planes.at[pl.ds(0, n_ma - 2)], p_send.at[1])
            await_all(planes.at[0], near_send)
            for where, count in ((hub_other, held), (jnp.logical_not(hub_other), splits)):
                @pl.when(where)
                def _():
                    await_all(planes.at[0, pl.ds(0, count)], p_send.at[2])

            @pl.when(hub_lead)
            def _():
                await_all(extra, x_send)

            @pl.when(hub_other)
            def _():
                await_all(beam_o, b_send.at[0])
                await_all(noise_o, b_send.at[1])
                with mark("incoming"):
                    await_all(incoming, i_recv)
                acc[:, end * lanes:] = incoming[...]
        else:
            await_all(planes.at[pl.ds(0, n_ma - 1)], p_send.at[1])
    with mark("heard"):
        await_all(slots.at[pl.ds(0, n_all - 1)], q_recv)

    per_freq = n_ma * n_pol
    tail = mark('tail'); tail.__enter__()
    masked, live, here = 0.0, 0.0, 0.0
    for f in range(n_freq):
        channel = jnp.sum(jnp.sum(slots[f * per_freq:(f + 1) * per_freq, 0, :], axis=0, keepdims=True), axis=1, keepdims=True) / total
        flag = slots[f * per_freq, 1:2, 0:1]
        masked += flag * channel
        live += flag
        here += jnp.where(freq == f, channel, 0.0)
    band = masked / live
    factor = mine[1:2, 0:1] / jnp.sqrt(0.5 * here + 0.5 * band + 1e-06)
    power_ref[...] = jnp.broadcast_to(here, power_ref.shape)
    scale_ref[...] = rs_n[...] * factor
    await_all(slots.at[pl.ds(0, n_all - 1)], q_send)
    if few:
        @pl.when(hub_lead)
        def _():
            await_all(acc_o, i_send)
    tail.__exit__(None,None,None)


def rescale_kernel(acc, scale_ref, power_ref, out_ref, channel_ref, staged, channel, sems, channel_sem):
    modes = scale_ref.shape[0]
    columns = acc.shape[1]
    strip = modes // sems.shape[0]
    channel[0] = power_ref[0, 0]
    last = pltpu.make_async_copy(channel, channel_ref, channel_sem)
    copies = []
    for i in range(sems.shape[0]):
        k0 = i * strip
        scale = scale_ref[k0:k0 + strip, :]
        for c in range(2):
            for j in range(columns // LANES):
                value = acc[c * modes + k0:c * modes + k0 + strip, j * LANES:(j + 1) * LANES]
                staged[c, k0:k0 + strip, j * LANES:(j + 1) * LANES] = (value * scale).astype(staged.dtype)
        copies.append(pltpu.make_async_copy(
            staged.at[:, pl.ds(k0, strip)], out_ref.at[:, pl.ds(k0, strip)], sems.at[i]))
        copies[-1].start()
        if i == 0:
            last.start()
    for copy in copies:
        copy.wait()
    last.wait()


def on_device(sizes, alm, beam, m_table, chan_mask, noise):
    n_ma, n_freq, n_pol = sizes
    coeffs = alm[:, 0]
    response = beam[0, 0]
    block, columns = coeffs.shape[1], coeffs.shape[3]
    modes, degrees = response.shape[1], response.shape[2]
    per_source = n_pol * block
    rows = per_source * max(1, min(n_ma, 256 // per_source))
    groups = degrees // rows
    splits = columns // LANES
    n_all = n_ma * n_freq * n_pol
    total = float(n_ma * modes * n_pol * columns)
    vmem = pl.BlockSpec(memory_space=pltpu.VMEM)
    hbm = pl.BlockSpec(memory_space=pltpu.HBM)
    smem = pl.BlockSpec(memory_space=pltpu.SMEM)
    dma = pltpu.SemaphoreType.DMA
    keep = functools.partial(pltpu.with_memory_space_constraint, memory_space=pltpu.HBM)
    visibility, scale, power = pl.pallas_call(
        functools.partial(step_kernel, sizes, total),
        out_shape=(
            jax.ShapeDtypeStruct((2 * modes, columns), jnp.float32),
            jax.ShapeDtypeStruct((modes, LANES), jnp.float32),
            jax.ShapeDtypeStruct((1, LANES), jnp.float32),
        ),
        in_specs=[hbm, hbm, smem, smem, hbm],
        out_specs=(vmem, vmem, vmem),
        scratch_shapes=[
            pltpu.VMEM((2, block, n_ma, columns), jnp.bfloat16),
            pltpu.VMEM((n_ma, splits, 2, block, LANES), jnp.bfloat16),
            pltpu.VMEM((2, 2, block, LANES), jnp.bfloat16),
            pltpu.VMEM((groups, splits, 2, rows, LANES), jnp.bfloat16),
            pltpu.VMEM((groups, 2 * modes, 2 * rows), jnp.bfloat16),
            pltpu.VMEM((groups, 2 * modes, 2 * rows), jnp.bfloat16),
            pltpu.VMEM((2, modes, degrees), jnp.bfloat16),
            pltpu.VMEM((2, modes, degrees), jnp.bfloat16),
            pltpu.VMEM((2 * modes, LANES), jnp.float32),
            pltpu.VMEM((2 * modes, LANES), jnp.float32),
            pltpu.VMEM((modes, LANES), jnp.float32),
            pltpu.VMEM((modes, LANES), jnp.float32),
            pltpu.VMEM((modes, LANES), jnp.float32),
            pltpu.VMEM((2, LANES), jnp.float32),
            pltpu.VMEM((n_all, 2, LANES), jnp.float32),
            pltpu.VMEM((8, LANES), jnp.float32),
            pltpu.VMEM((1, modes), jnp.float32),
            pltpu.VMEM((1, modes), jnp.float32),
            dma, dma, dma, dma, dma((2,)), dma((2,)), dma, dma,
            dma((n_ma,)), dma((splits,)), dma((2,)), dma((3,)), dma((n_ma,)), dma((splits,)),
            dma((splits,)), dma, dma, dma,
            pltpu.SemaphoreType.REGULAR((2,)), pltpu.SemaphoreType.REGULAR((2,)), dma,
        ],
        compiler_params=pltpu.CompilerParams(collective_id=0, has_side_effects=True, vmem_limit_bytes=40 * 1024 * 1024),
        name="driftscan_step",
    )(keep(coeffs), keep(response), m_table, chan_mask, keep(noise))
    pieces = 8 if modes % 128 == 0 else 1
    scaled, channel_power = pl.pallas_call(
        rescale_kernel,
        out_shape=(
            jax.ShapeDtypeStruct((2, modes, columns), jnp.bfloat16),
            jax.ShapeDtypeStruct((1,), jnp.float32),
        ),
        in_specs=[vmem, vmem, vmem],
        out_specs=(hbm, hbm),
        scratch_shapes=[pltpu.VMEM((2, modes, columns), jnp.bfloat16), pltpu.SMEM((1,), jnp.float32), dma((pieces,)), dma],
        compiler_params=pltpu.CompilerParams(vmem_limit_bytes=16 * 1024 * 1024),
        name="rescale",
    )(visibility, scale, power)
    return scaled[:, None, None], channel_power


def solution(mesh):
    sizes = (mesh.shape["ma"], mesh.shape["freq"], mesh.shape["pol"])
    return jax.shard_map(
        functools.partial(on_device, sizes),
        mesh=mesh,
        in_specs=(
            P(None, "freq", ("ma", "pol"), None, "sky"),
            P("ma", "freq", None, "pol", None),
            P("ma"),
            P("freq"),
            P("freq", "pol"),
        ),
        out_specs=(P(None, "freq", "ma", "pol", "sky"), P(("sky", "freq"))),
        check_vma=False,
    )
```

```python
import contextlib
import functools

import jax
import jax.numpy as jnp
from jax import lax
from jax.experimental import pallas as pl
from jax.experimental.pallas import tpu as pltpu
from jax.sharding import PartitionSpec as P

MESH = pl.DeviceIdType.MESH
LANES = 128


def mark(name):
    return contextlib.nullcontext()


def across(n, i):
    return n // 2 if 2 * i < n else n // 2 - 1


def processing_order(n, i):
    last = across(n, i)
    rest = sorted((j for j in range(n) if j not in (i, last)), key=lambda j: (-abs(j - i), j))
    return rest + ([last] if last != i else [])


def far_first(n, i):
    return sorted((j for j in range(n) if j != i), key=lambda j: (-abs(j - i), j != across(n, i), j))


def pick_by(me, values):
    pick = jnp.int32(values[0])
    for i in range(1, len(values)):
        pick = jnp.where(me == i, jnp.int32(values[i]), pick)
    return pick


def step_kernel(
    sizes, total, alm_hbm, beam_hbm, m_ref, mask_ref, noise_hbm, acc, scale_ref, power_ref,
    staged, planes, extra, guest, recv, wide, wide_o, beam_v, beam_o, acc_o, incoming, inv_n, inv_o, rs_n, mine, slots, total_ref,
    noise_ref, noise_o,
    z_send, near_send, g_send, g_recv, x_send, x_recv, b_send, b_recv, i_send, i_recv, z_far, z_last, y_last, p_send, p_far, p_last, in_sem, beam_sem, q_send, q_recv, edge, meet, small_sem,
):
    n_ma, n_freq, n_pol = sizes
    n_all = n_ma * n_freq * n_pol
    ma, freq, pol = lax.axis_index("ma"), lax.axis_index("freq"), lax.axis_index("pol")
    block = staged.shape[1]
    groups, splits, _, rows, lanes = recv.shape
    per_source = n_pol * block
    per_group = rows // per_source
    modes = beam_hbm.shape[1]
    my_slot = (freq * n_ma + ma) * n_pol + pol
    few = 2 < n_ma <= 8 and per_group == 1 and n_pol == 2 and block % LANES == 0 and splits > 3

    def place(slot):
        return {"ma": lax.rem(slot // n_pol, n_ma), "freq": slot // (n_pol * n_ma), "pol": lax.rem(slot, n_pol)}

    def loop(low, high, body, unroll=False):
        if unroll:
            for r in range(low, high):
                body(r)
        else:
            lax.fori_loop(low, high, lambda r, _: (body(r), 0)[1], 0)

    def for_peers(body):
        loop(1, n_all, body, n_all <= 32)

    barrier = pltpu.get_barrier_semaphore()

    def tell(axis, me, n, sem):
        loop(1, n, lambda q: pl.semaphore_signal(
            sem, inc=1, device_id={axis: lax.rem(me + q, n)}, device_id_type=MESH), n <= 8)

    low = n_ma // 2
    below = ma < low
    inward, outward = jnp.where(below, ma + 1, ma - 1), jnp.where(below, ma - 1, ma + 1)
    is_hub = jnp.logical_or(ma == low - 1, ma == low)
    has_outward = jnp.logical_and(ma > 0, ma < n_ma - 1)
    odd = lax.rem(freq, 2) == 1
    hub_lead, hub_other = jnp.logical_and(is_hub, pol == 1), jnp.logical_and(is_hub, pol == 0)

    def tell_line(there, sem):
        pl.semaphore_signal(sem, inc=1, device_id={"ma": there}, device_id_type=MESH)

    @pl.when(is_hub)
    def _():
        tell_line(inward, barrier)

    @pl.when(has_outward)
    def _():
        tell_line(outward, barrier)

    tell("pol", pol, n_pol, barrier)
    tell("freq", freq, n_freq, barrier)

    def columns_of(j):
        return pl.ds(j * lanes, lanes)

    loads = [pltpu.make_async_copy(alm_hbm.at[:, :, :, columns_of(j)], staged.at[:, :, :, columns_of(j)], in_sem.at[j])
             for j in range(splits)]
    for load in loads:
        load.start()
    noise_copy = pltpu.make_async_copy(noise_hbm, noise_ref, small_sem)
    beam_copy = pltpu.make_async_copy(beam_hbm, beam_v, beam_sem)

    def part(source, core, j):
        start = lax.rem(source, per_group) * per_source + core * block
        return recv.at[source // per_group, j, :, pl.ds(pl.multiple_of(start, block), block)]

    is_end = jnp.logical_not(jnp.logical_or(is_hub, has_outward))

    def enter():
        pl.semaphore_wait(barrier, 1 + n_pol - 1 + n_freq - 1)

    @pl.when(is_end)
    def _():
        enter()
        tell_line(inward, edge.at[0])

    step = min(block, 16)

    def turn(j):
        with mark("load"):
            loads[j].wait()
        for c in range(2):
            for e in range(0, block, step):
                planes[:, j, c, e:e + step, :] = jnp.transpose(staged[c, e:e + step, :, columns_of(j)], (1, 0, 2))

    turn(0)
    with mark("barrier"):
        @pl.when(jnp.logical_not(is_end))
        def _():
            enter()

    def push(src, dst, sent, got, where):
        pltpu.make_async_remote_copy(
            src_ref=src, dst_ref=dst, send_sem=sent, recv_sem=got, device_id=where, device_id_type=MESH).start()

    def send(target, j, got, sent):
        push(planes.at[target, j], part(ma, pol, j), sent, got, {"ma": target})

    def whole(source, core):
        start = lax.rem(source, per_group) * per_source + core * block
        return recv.at[source // per_group, :, :, pl.ds(pl.multiple_of(start, block), block)]

    def await_all(ref, sem):
        pltpu.make_async_copy(ref, ref, sem).wait()

    def relay(source, j, sent, got, src=None):
        for q in range(1, n_pol):
            push(part(source, pol, j) if src is None else src, part(source, pol, j), sent, got,
                 {"pol": lax.rem(pol + q, n_pol)})

    def relayed(source):
        for q in range(1, n_pol):
            await_all(whole(source, lax.rem(pol + q, n_pol)), p_far.at[source])

    held = splits - 2

    def send_phase(phase):
        for i in range(n_ma):
            near = i + 1 if i < low else i - 1
            outer = range(0, i) if i < low else range(i + 1, n_ma)
            plan = [(t, j) for t in far_first(n_ma, i) for j in range(splits)]
            first = [(near, j) for j in range(2)]
            second = [(t, j) for t, j in plan if t in outer]
            rest = [step for step in plan if step not in first + second]
            hub = i in (low - 1, low)
            now = (first[:1], first[1:], second, rest)[phase]
            late = [(t, j) for t, j in now if hub and t == near and j >= held]
            if now:
                @pl.when(ma == i)
                def _():
                    def go(t, j):
                        send(t, j, z_last.at[j] if i == across(n_ma, t) else z_far.at[i],
                             near_send if t == near else z_send)

                    for t, j in now:
                        if hub and (t, j) == (near, 1):
                            detour = jnp.logical_and(odd, pol == 1)

                            @pl.when(detour)
                            def _():
                                push(planes.at[t, j, 0], guest, near_send, g_recv, {"freq": freq - 1})
                                push(planes.at[t, j, 1], part(ma, pol, j).at[1], near_send, z_last.at[j], {"ma": t})

                            @pl.when(jnp.logical_not(detour))
                            def _():
                                go(t, j)
                        elif (t, j) not in late:
                            go(t, j)
                    if late:
                        @pl.when(pol == 0)
                        def _():
                            push(planes.at[near, pl.ds(held, 2)], extra, near_send, x_recv, {"pol": 1})

                        @pl.when(pol == 1)
                        def _():
                            await_all(extra, x_recv)
                            for t, j in late:
                                push(extra.at[j - held], part(ma, 0, j), x_send, y_last.at[j - held], {"ma": t})
                                send(t, j, z_last.at[j], near_send)

    has_guest = jnp.logical_and(hub_lead, jnp.logical_and(jnp.logical_not(odd), freq < n_freq - 1))

    def forward_guest():
        @pl.when(has_guest)
        def _():
            await_all(guest, g_recv)
            push(guest, part(ma, pol, 1).at[0], g_send, z_last.at[1], {"ma": inward, "freq": freq + 1})

    if few:
        send_phase(0)
    for j in range(1, splits):
        turn(j)
        if few and j == 1:
            send_phase(1)
    noise_copy.start()
    beam_copy.start()

    with mark("edge0"):
        @pl.when(has_outward)
        def _():
            pl.semaphore_wait(edge.at[0], 1)

    @pl.when(is_hub)
    def _():
        tell_line(inward, edge.at[1])

    @pl.when(jnp.logical_and(has_outward, jnp.logical_not(is_hub)))
    def _():
        tell_line(inward, edge.at[0])

    if few:
        send_phase(2)
    with mark("edge1"):
        pl.semaphore_wait(edge.at[1], 1)

    @pl.when(has_outward)
    def _():
        tell_line(outward, edge.at[1])

    if few:
        forward_guest()
        send_phase(3)
    else:
        for j in range(splits):
            loop(1, n_ma, lambda q: send(lax.rem(ma + q, n_ma), j, z_far.at[ma], z_send))

    for j in range(splits):
        relay(ma, j, p_send.at[0], p_far.at[ma], planes.at[ma, j])
        for c in range(2):
            part(ma, pol, j)[c] = planes[ma, j, c]

    if few:
        @pl.when(hub_other)
        def _():
            push(beam_hbm, beam_o, b_send.at[0], b_recv.at[0], {"pol": 1})
            push(noise_hbm, noise_o, b_send.at[1], b_recv.at[1], {"pol": 1})

    noise_copy.wait()
    spread = jnp.transpose(jnp.broadcast_to(noise_ref[...], (LANES, modes)))
    inv_n[...] = 1.0 / spread
    rs_n[...] = lax.rsqrt(spread)
    mine[1:2, :] = jnp.full((1, LANES), mask_ref[0].astype(jnp.float32))
    beam_copy.wait()
    strip = min(modes, 128)

    def widen(beam_v, wide, i):
        k0 = pl.multiple_of(i * strip, strip)
        for g in range(groups):
            degree = lax.broadcasted_iota(jnp.int32, (strip, rows), 1) + g * rows
            keep = degree >= m_ref[0]
            zero = jnp.zeros((strip, rows), jnp.float32)
            b0 = jnp.where(keep, beam_v[0, pl.ds(k0, strip), g * rows:(g + 1) * rows].astype(jnp.float32), zero)
            b1 = jnp.where(keep, beam_v[1, pl.ds(k0, strip), g * rows:(g + 1) * rows].astype(jnp.float32), zero)
            wide[g, pl.ds(k0, strip), 0:rows] = b0.astype(wide.dtype)
            wide[g, pl.ds(k0, strip), rows:2 * rows] = (-b1).astype(wide.dtype)
            wide[g, pl.ds(modes + k0, strip), 0:rows] = b1.astype(wide.dtype)
            wide[g, pl.ds(modes + k0, strip), rows:2 * rows] = b0.astype(wide.dtype)

    with mark("widen"):
        loop(0, modes // strip, functools.partial(widen, beam_v, wide))
    tell("pol", pol, n_pol, meet.at[0])
    pl.semaphore_wait(meet.at[0], n_pol - 1)
    tell("freq", freq, n_freq, meet.at[1])
    pl.semaphore_wait(meet.at[1], n_freq - 1)

    if few:
        @pl.when(hub_lead)
        def _():
            await_all(noise_o, b_recv.at[1])
            inv_o[...] = 1.0 / jnp.transpose(jnp.broadcast_to(noise_o[...], (LANES, modes)))
            await_all(beam_o, b_recv.at[0])
            loop(0, modes // strip, functools.partial(widen, beam_o, wide_o))

    tile = min(modes, 256)

    def add(g, first=False):
        x = jnp.concatenate([recv[g, j].reshape(2 * rows, lanes) for j in range(splits)], axis=1)

        def body(k0):
            value = jnp.dot(wide[g, pl.ds(k0, tile), :], x, preferred_element_type=jnp.float32)
            acc[pl.ds(k0, tile), :] = value if first else acc[pl.ds(k0, tile), :] + value

        for i in range(2 * modes // tile):
            body(i * tile)

    def half(w, g, j, core):
        start = pl.multiple_of(core * block, block)
        x = jnp.concatenate([recv[g, j, c, pl.ds(start, block), :] for c in range(2)], axis=0)

        def value(k0):
            left = jnp.concatenate([w[g, k0:k0 + tile, pl.ds(pl.multiple_of(c * rows + start, block), block)]
                                    for c in range(2)], axis=1)
            return jnp.dot(left, x, preferred_element_type=jnp.float32)
        return value

    def full(w, g, j):
        x = recv[g, j].reshape(2 * rows, lanes)
        return lambda k0: jnp.dot(w[g, k0:k0 + tile, :], x, preferred_element_type=jnp.float32)

    def add_to(sums, j, product, first=False):
        for i in range(2 * modes // tile):
            at = (slice(i * tile, (i + 1) * tile), slice(j * lanes, (j + 1) * lanes))
            sums[at] = product(i * tile) if first else sums[at] + product(i * tile)

    def finish(sums, weights, j, product=None):
        power = total_ref[...]
        for i in range(2 * modes // tile):
            at = (slice(i * tile, (i + 1) * tile), slice(j * lanes, (j + 1) * lanes))
            value = sums[at]
            if product is not None:
                value = value + product(i * tile)
                sums[at] = value
            k0 = i * tile % modes
            weighted = value * value * weights[k0:k0 + tile, :]
            power = power + jnp.sum(weighted.reshape(tile // 8, 8, lanes), axis=0)
        total_ref[...] = power

    def finish_both(product, product_o):
        power, power_o = total_ref[...], jnp.zeros(total_ref.shape, jnp.float32)
        for i in range(2 * modes // tile):
            row, k0 = slice(i * tile, (i + 1) * tile), i * tile % modes
            value_o = acc_o[row, :] + product_o(i * tile)
            value = acc[row, (splits - 1) * lanes:] + product(i * tile)
            acc_o[row, :] = value_o
            acc[row, (splits - 1) * lanes:] = value
            power_o = power_o + jnp.sum((value_o * value_o * inv_o[k0:k0 + tile, :]).reshape(tile // 8, 8, lanes), axis=0)
            power = power + jnp.sum((value * value * inv_n[k0:k0 + tile, :]).reshape(tile // 8, 8, lanes), axis=0)
        total_ref[...] = power + power_o

    total_ref[...] = jnp.zeros_like(total_ref)
    if few:
        order = [pick_by(ma, [processing_order(n_ma, i)[k] for i in range(n_ma)]) for k in range(n_ma - 1)]
        last, end = order[-1], splits - 1

        def own_block(j):
            with mark(f"last{j}"):
                await_all(part(last, pol, j), z_last.at[j])

        def other_block(j):
            with mark(f"hop{j}"):
                await_all(part(last, 1 - pol, j), p_last.at[j])

        def pass_block(j, core=None, slot=None):
            at = part(last, pol if core is None else core, j)
            push(at, at, p_send.at[2], p_last.at[j if slot is None else slot], {"pol": 1 - pol})

        def take(k):
            with mark(f"wait{k}"):
                await_all(whole(order[k], pol), z_far.at[order[k]])
            for j in range(splits):
                relay(order[k], j, p_send.at[1], p_far.at[order[k]])

        def settle(source, first=False, shared=False):
            with mark("relay"):
                relayed(source)
            with mark("add"):
                add(source, first)
                if shared:
                    @pl.when(hub_lead)
                    def _():
                        add_to(acc_o, 0, full(wide_o, source, end), first)

        @pl.when(is_hub)
        def _():
            for j in range(held):
                own_block(j)
                pass_block(j)
            settle(ma, True, True)
            for j in range(held):
                other_block(j)
                add_to(acc, j, full(wide, last, j))
            for k in range(n_ma - 2):
                take(k)
                if k:
                    settle(order[k - 1], False, True)
            if n_ma > 2:
                settle(order[n_ma - 3], False, True)

        @pl.when(hub_lead)
        def _():
            with mark("y0"):
                await_all(part(last, 0, held), y_last.at[0])
            pass_block(held, 0, end)
            own_block(held)
            pass_block(held)
            for j in range(held):
                finish(acc, inv_n, j)
            finish(acc, inv_n, held, full(wide, last, held))
            with mark("y1"):
                await_all(part(last, 0, end), y_last.at[1])
            add_to(acc, end, half(wide, last, end, 0))
            add_to(acc_o, 0, half(wide_o, last, end, 0))
            own_block(end)
            finish_both(half(wide, last, end, 1), half(wide_o, last, end, 1))

        @pl.when(hub_other)
        def _():
            for j in range(held):
                finish(acc, inv_n, j)
            with mark("x"):
                await_all(part(last, 0, held), p_last.at[end])
            other_block(held)
            finish(acc, inv_n, held, full(wide, last, held))

        @pl.when(jnp.logical_not(is_hub))
        def _():
            before = ma
            for k in range(n_ma - 2):
                take(k)
                settle(before, k == 0)
                before = order[k]
            own_block(0)
            pass_block(0)
            settle(before)
            add_to(acc, 0, half(wide, last, 0, pol))
            for j in range(1, splits):
                own_block(j)
                pass_block(j)
                add_to(acc, j, half(wide, last, j, pol))
                other_block(j - 1)
                finish(acc, inv_n, j - 1, half(wide, last, j - 1, 1 - pol))
            other_block(end)
            finish(acc, inv_n, end, half(wide, last, end, 1 - pol))
    else:
        def pass_on(source):
            @pl.when(source != ma)
            def _():
                await_all(whole(source, pol), z_far.at[source])
                for j in range(splits):
                    relay(source, j, p_send.at[1], p_far.at[source])
        loop(0, n_ma, pass_on)
        loop(0, n_ma, relayed)
        for g in range(groups):
            add(g, g == 0)
        for j in range(splits):
            finish(acc, inv_n, j)

    row = jnp.sum(total_ref[...], axis=0, keepdims=True)
    mine[0:1, :] = row
    slots[my_slot, 0:1, :] = row
    slots[my_slot, 1:2, :] = mine[1:2, :]

    def report(r):
        pltpu.make_async_remote_copy(
            src_ref=mine, dst_ref=slots.at[my_slot], send_sem=q_send, recv_sem=q_recv,
            device_id=place(lax.rem(my_slot + r, n_all)), device_id_type=MESH).start()

    for_peers(report)
    if few:
        @pl.when(hub_lead)
        def _():
            push(acc_o, incoming, i_send, i_recv, {"pol": 0})

    with mark("drain"):
        await_all(planes.at[pl.ds(0, n_ma - 2 if few else n_ma - 1)], z_send)
        await_all(planes.at[0], p_send.at[0])
        if few:
            if n_ma > 2:
                await_all(planes.at[pl.ds(0, n_ma - 2)], p_send.at[1])
            await_all(planes.at[0], near_send)
            for where, count in ((hub_other, held), (jnp.logical_not(hub_other), splits)):
                @pl.when(where)
                def _():
                    await_all(planes.at[0, pl.ds(0, count)], p_send.at[2])

            @pl.when(hub_lead)
            def _():
                await_all(extra, x_send)

            @pl.when(has_guest)
            def _():
                await_all(guest, g_send)

            @pl.when(hub_other)
            def _():
                await_all(beam_o, b_send.at[0])
                await_all(noise_o, b_send.at[1])
                with mark("incoming"):
                    await_all(incoming, i_recv)
                acc[:, end * lanes:] = incoming[...]
        else:
            await_all(planes.at[pl.ds(0, n_ma - 1)], p_send.at[1])
    with mark("heard"):
        await_all(slots.at[pl.ds(0, n_all - 1)], q_recv)

    per_freq = n_ma * n_pol
    tail = mark('tail'); tail.__enter__()
    masked, live, here = 0.0, 0.0, 0.0
    for f in range(n_freq):
        channel = jnp.sum(jnp.sum(slots[f * per_freq:(f + 1) * per_freq, 0, :], axis=0, keepdims=True), axis=1, keepdims=True) / total
        flag = slots[f * per_freq, 1:2, 0:1]
        masked += flag * channel
        live += flag
        here += jnp.where(freq == f, channel, 0.0)
    band = masked / live
    factor = mine[1:2, 0:1] / jnp.sqrt(0.5 * here + 0.5 * band + 1e-06)
    power_ref[...] = jnp.broadcast_to(here, power_ref.shape)
    scale_ref[...] = rs_n[...] * factor
    await_all(slots.at[pl.ds(0, n_all - 1)], q_send)
    if few:
        @pl.when(hub_lead)
        def _():
            await_all(acc_o, i_send)
    tail.__exit__(None,None,None)


def rescale_kernel(acc, scale_ref, power_ref, out_ref, channel_ref, staged, channel, sems, channel_sem):
    modes = scale_ref.shape[0]
    columns = acc.shape[1]
    strip = modes // sems.shape[0]
    channel[0] = power_ref[0, 0]
    last = pltpu.make_async_copy(channel, channel_ref, channel_sem)
    copies = []
    for i in range(sems.shape[0]):
        k0 = i * strip
        scale = scale_ref[k0:k0 + strip, :]
        for c in range(2):
            for j in range(columns // LANES):
                value = acc[c * modes + k0:c * modes + k0 + strip, j * LANES:(j + 1) * LANES]
                staged[c, k0:k0 + strip, j * LANES:(j + 1) * LANES] = (value * scale).astype(staged.dtype)
        copies.append(pltpu.make_async_copy(
            staged.at[:, pl.ds(k0, strip)], out_ref.at[:, pl.ds(k0, strip)], sems.at[i]))
        copies[-1].start()
        if i == 0:
            last.start()
    for copy in copies:
        copy.wait()
    last.wait()


def on_device(sizes, alm, beam, m_table, chan_mask, noise):
    n_ma, n_freq, n_pol = sizes
    coeffs = alm[:, 0]
    response = beam[0, 0]
    block, columns = coeffs.shape[1], coeffs.shape[3]
    modes, degrees = response.shape[1], response.shape[2]
    per_source = n_pol * block
    rows = per_source * max(1, min(n_ma, 256 // per_source))
    groups = degrees // rows
    splits = columns // LANES
    n_all = n_ma * n_freq * n_pol
    total = float(n_ma * modes * n_pol * columns)
    vmem = pl.BlockSpec(memory_space=pltpu.VMEM)
    hbm = pl.BlockSpec(memory_space=pltpu.HBM)
    smem = pl.BlockSpec(memory_space=pltpu.SMEM)
    dma = pltpu.SemaphoreType.DMA
    keep = functools.partial(pltpu.with_memory_space_constraint, memory_space=pltpu.HBM)
    visibility, scale, power = pl.pallas_call(
        functools.partial(step_kernel, sizes, total),
        out_shape=(
            jax.ShapeDtypeStruct((2 * modes, columns), jnp.float32),
            jax.ShapeDtypeStruct((modes, LANES), jnp.float32),
            jax.ShapeDtypeStruct((1, LANES), jnp.float32),
        ),
        in_specs=[hbm, hbm, smem, smem, hbm],
        out_specs=(vmem, vmem, vmem),
        scratch_shapes=[
            pltpu.VMEM((2, block, n_ma, columns), jnp.bfloat16),
            pltpu.VMEM((n_ma, splits, 2, block, LANES), jnp.bfloat16),
            pltpu.VMEM((2, 2, block, LANES), jnp.bfloat16),
            pltpu.VMEM((block, LANES), jnp.bfloat16),
            pltpu.VMEM((groups, splits, 2, rows, LANES), jnp.bfloat16),
            pltpu.VMEM((groups, 2 * modes, 2 * rows), jnp.bfloat16),
            pltpu.VMEM((groups, 2 * modes, 2 * rows), jnp.bfloat16),
            pltpu.VMEM((2, modes, degrees), jnp.bfloat16),
            pltpu.VMEM((2, modes, degrees), jnp.bfloat16),
            pltpu.VMEM((2 * modes, LANES), jnp.float32),
            pltpu.VMEM((2 * modes, LANES), jnp.float32),
            pltpu.VMEM((modes, LANES), jnp.float32),
            pltpu.VMEM((modes, LANES), jnp.float32),
            pltpu.VMEM((modes, LANES), jnp.float32),
            pltpu.VMEM((2, LANES), jnp.float32),
            pltpu.VMEM((n_all, 2, LANES), jnp.float32),
            pltpu.VMEM((8, LANES), jnp.float32),
            pltpu.VMEM((1, modes), jnp.float32),
            pltpu.VMEM((1, modes), jnp.float32),
            dma, dma, dma, dma, dma, dma, dma((2,)), dma((2,)), dma, dma,
            dma((n_ma,)), dma((splits,)), dma((2,)), dma((3,)), dma((n_ma,)), dma((splits,)),
            dma((splits,)), dma, dma, dma,
            pltpu.SemaphoreType.REGULAR((2,)), pltpu.SemaphoreType.REGULAR((2,)), dma,
        ],
        compiler_params=pltpu.CompilerParams(collective_id=0, has_side_effects=True, vmem_limit_bytes=40 * 1024 * 1024),
        name="driftscan_step",
    )(keep(coeffs), keep(response), m_table, chan_mask, keep(noise))
    pieces = 8 if modes % 128 == 0 else 1
    scaled, channel_power = pl.pallas_call(
        rescale_kernel,
        out_shape=(
            jax.ShapeDtypeStruct((2, modes, columns), jnp.bfloat16),
            jax.ShapeDtypeStruct((1,), jnp.float32),
        ),
        in_specs=[vmem, vmem, vmem],
        out_specs=(hbm, hbm),
        scratch_shapes=[pltpu.VMEM((2, modes, columns), jnp.bfloat16), pltpu.SMEM((1,), jnp.float32), dma((pieces,)), dma],
        compiler_params=pltpu.CompilerParams(vmem_limit_bytes=16 * 1024 * 1024),
        name="rescale",
    )(visibility, scale, power)
    return scaled[:, None, None], channel_power


def solution(mesh):
    sizes = (mesh.shape["ma"], mesh.shape["freq"], mesh.shape["pol"])
    return jax.shard_map(
        functools.partial(on_device, sizes),
        mesh=mesh,
        in_specs=(
            P(None, "freq", ("ma", "pol"), None, "sky"),
            P("ma", "freq", None, "pol", None),
            P("ma"),
            P("freq"),
            P("freq", "pol"),
        ),
        out_specs=(P(None, "freq", "ma", "pol", "sky"), P(("sky", "freq"))),
        check_vma=False,
    )
```

```python
import contextlib
import functools

import jax
import jax.numpy as jnp
from jax import lax
from jax.experimental import pallas as pl
from jax.experimental.pallas import tpu as pltpu
from jax.sharding import PartitionSpec as P

MESH = pl.DeviceIdType.MESH
LANES = 128


def mark(name):
    return contextlib.nullcontext()


def across(n, i):
    return n // 2 if 2 * i < n else n // 2 - 1


def processing_order(n, i):
    last = across(n, i)
    rest = sorted((j for j in range(n) if j not in (i, last)), key=lambda j: (-abs(j - i), j))
    return rest + ([last] if last != i else [])


def far_first(n, i):
    return sorted((j for j in range(n) if j != i), key=lambda j: (-abs(j - i), j != across(n, i), j))


def pick_by(me, values):
    pick = jnp.int32(values[0])
    for i in range(1, len(values)):
        pick = jnp.where(me == i, jnp.int32(values[i]), pick)
    return pick


def step_kernel(
    sizes, total, alm_hbm, beam_hbm, m_ref, mask_ref, noise_hbm, acc, scale_ref, power_ref,
    staged, planes, extra, guest, recv, wide, wide_o, beam_v, beam_o, acc_o, incoming, inv_n, inv_o, rs_n, mine, slots, total_ref,
    noise_ref, noise_o,
    z_send, near_send, g_send, g_recv, c_send, c_recv, z_far, z_last, p_send, p_far, p_last, in_sem, beam_sem, q_send, q_recv, edge, meet, small_sem,
):
    n_ma, n_freq, n_pol = sizes
    n_all = n_ma * n_freq * n_pol
    ma, freq, pol = lax.axis_index("ma"), lax.axis_index("freq"), lax.axis_index("pol")
    block = staged.shape[1]
    groups, splits, _, rows, lanes = recv.shape
    per_source = n_pol * block
    per_group = rows // per_source
    modes = beam_hbm.shape[1]
    my_slot = (freq * n_ma + ma) * n_pol + pol
    few = 2 < n_ma <= 8 and per_group == 1 and n_pol == 2 and block % LANES == 0 and splits > 3

    def place(slot):
        return {"ma": lax.rem(slot // n_pol, n_ma), "freq": slot // (n_pol * n_ma), "pol": lax.rem(slot, n_pol)}

    def loop(low, high, body, unroll=False):
        if unroll:
            for r in range(low, high):
                body(r)
        else:
            lax.fori_loop(low, high, lambda r, _: (body(r), 0)[1], 0)

    def for_peers(body):
        loop(1, n_all, body, n_all <= 32)

    barrier = pltpu.get_barrier_semaphore()

    def tell(axis, me, n, sem):
        loop(1, n, lambda q: pl.semaphore_signal(
            sem, inc=1, device_id={axis: lax.rem(me + q, n)}, device_id_type=MESH), n <= 8)

    low = n_ma // 2
    below = ma < low
    inward, outward = jnp.where(below, ma + 1, ma - 1), jnp.where(below, ma - 1, ma + 1)
    is_hub = jnp.logical_or(ma == low - 1, ma == low)
    has_outward = jnp.logical_and(ma > 0, ma < n_ma - 1)
    odd = lax.rem(freq, 2) == 1
    hub_lead, hub_other = jnp.logical_and(is_hub, pol == 1), jnp.logical_and(is_hub, pol == 0)

    def tell_line(there, sem):
        pl.semaphore_signal(sem, inc=1, device_id={"ma": there}, device_id_type=MESH)

    @pl.when(is_hub)
    def _():
        tell_line(inward, barrier)

    @pl.when(has_outward)
    def _():
        tell_line(outward, barrier)

    tell("pol", pol, n_pol, barrier)
    tell("freq", freq, n_freq, barrier)

    def columns_of(j):
        return pl.ds(j * lanes, lanes)

    loads = [pltpu.make_async_copy(alm_hbm.at[:, :, :, columns_of(j)], staged.at[:, :, :, columns_of(j)], in_sem.at[j])
             for j in range(splits)]
    for load in loads:
        load.start()
    noise_copy = pltpu.make_async_copy(noise_hbm, noise_ref, small_sem)
    beam_copy = pltpu.make_async_copy(beam_hbm, beam_v, beam_sem)

    def part(source, core, j):
        start = lax.rem(source, per_group) * per_source + core * block
        return recv.at[source // per_group, j, :, pl.ds(pl.multiple_of(start, block), block)]

    is_end = jnp.logical_not(jnp.logical_or(is_hub, has_outward))

    def enter():
        pl.semaphore_wait(barrier, 1 + n_pol - 1 + n_freq - 1)

    @pl.when(is_end)
    def _():
        enter()
        tell_line(inward, edge.at[0])

    step = min(block, 16)

    def turn(j):
        with mark("load"):
            loads[j].wait()
        for c in range(2):
            for e in range(0, block, step):
                planes[:, j, c, e:e + step, :] = jnp.transpose(staged[c, e:e + step, :, columns_of(j)], (1, 0, 2))

    turn(0)
    with mark("barrier"):
        @pl.when(jnp.logical_not(is_end))
        def _():
            enter()

    def push(src, dst, sent, got, where):
        pltpu.make_async_remote_copy(
            src_ref=src, dst_ref=dst, send_sem=sent, recv_sem=got, device_id=where, device_id_type=MESH).start()

    def send(target, j, got, sent):
        push(planes.at[target, j], part(ma, pol, j), sent, got, {"ma": target})

    def whole(source, core):
        start = lax.rem(source, per_group) * per_source + core * block
        return recv.at[source // per_group, :, :, pl.ds(pl.multiple_of(start, block), block)]

    def await_all(ref, sem):
        pltpu.make_async_copy(ref, ref, sem).wait()

    def relay(source, j, sent, got, src=None):
        for q in range(1, n_pol):
            push(part(source, pol, j) if src is None else src, part(source, pol, j), sent, got,
                 {"pol": lax.rem(pol + q, n_pol)})

    def relayed(source):
        for q in range(1, n_pol):
            await_all(whole(source, lax.rem(pol + q, n_pol)), p_far.at[source])

    held = splits - 2

    def send_phase(phase):
        for i in range(n_ma):
            near = i + 1 if i < low else i - 1
            outer = range(0, i) if i < low else range(i + 1, n_ma)
            plan = [(t, j) for t in far_first(n_ma, i) for j in range(splits)]
            first = [(near, j) for j in range(2)]
            second = [(t, j) for t, j in plan if t in outer]
            rest = [step for step in plan if step not in first + second]
            hub = i in (low - 1, low)
            now = (first[:1], first[1:], second, rest)[phase]
            late = [(t, j) for t, j in now if hub and t == near and j >= held]
            if now:
                @pl.when(ma == i)
                def _():
                    def go(t, j):
                        send(t, j, z_last.at[j] if i == across(n_ma, t) else z_far.at[i],
                             near_send if t == near else z_send)

                    for t, j in now:
                        if hub and (t, j) == (near, 1):
                            detour = jnp.logical_and(odd, pol == 1)

                            @pl.when(detour)
                            def _():
                                push(planes.at[t, j, 0], guest, near_send, g_recv, {"freq": freq - 1})
                                push(planes.at[t, j, 1], part(ma, pol, j).at[1], near_send, z_last.at[j], {"ma": t})

                            @pl.when(jnp.logical_not(detour))
                            def _():
                                go(t, j)
                        elif (t, j) not in late:
                            go(t, j)
                    if late:
                        @pl.when(pol == 0)
                        def _():
                            push(planes.at[near, pl.ds(held, 2)], extra, near_send, c_recv.at[2], {"pol": 1})

                        @pl.when(pol == 1)
                        def _():
                            await_all(extra, c_recv.at[2])
                            for t, j in late:
                                push(extra.at[j - held], part(ma, 0, j), c_send.at[0], p_last.at[j], {"ma": t})
                                send(t, j, z_last.at[j], near_send)

    has_guest = jnp.logical_and(hub_lead, jnp.logical_and(jnp.logical_not(odd), freq < n_freq - 1))

    def forward_guest():
        @pl.when(has_guest)
        def _():
            await_all(guest, g_recv)
            push(guest, part(ma, pol, 1).at[0], g_send, z_last.at[1], {"ma": inward, "freq": freq + 1})

    if few:
        send_phase(0)
    for j in range(1, splits):
        turn(j)
        if few and j == 1:
            send_phase(1)
    noise_copy.start()
    beam_copy.start()

    with mark("edge0"):
        @pl.when(has_outward)
        def _():
            pl.semaphore_wait(edge.at[0], 1)

    @pl.when(is_hub)
    def _():
        tell_line(inward, edge.at[1])

    @pl.when(jnp.logical_and(has_outward, jnp.logical_not(is_hub)))
    def _():
        tell_line(inward, edge.at[0])

    if few:
        send_phase(2)
    with mark("edge1"):
        pl.semaphore_wait(edge.at[1], 1)

    @pl.when(has_outward)
    def _():
        tell_line(outward, edge.at[1])

    if few:
        forward_guest()
        send_phase(3)
    else:
        for j in range(splits):
            loop(1, n_ma, lambda q: send(lax.rem(ma + q, n_ma), j, z_far.at[ma], z_send))

    for j in range(splits):
        relay(ma, j, p_send.at[0], p_far.at[ma], planes.at[ma, j])
        for c in range(2):
            part(ma, pol, j)[c] = planes[ma, j, c]

    if few:
        @pl.when(hub_other)
        def _():
            push(beam_hbm, beam_o, c_send.at[0], c_recv.at[0], {"pol": 1})
            push(noise_hbm, noise_o, c_send.at[1], c_recv.at[1], {"pol": 1})

    noise_copy.wait()
    spread = jnp.transpose(jnp.broadcast_to(noise_ref[...], (LANES, modes)))
    inv_n[...] = 1.0 / spread
    rs_n[...] = lax.rsqrt(spread)
    mine[1:2, :] = jnp.full((1, LANES), mask_ref[0].astype(jnp.float32))
    beam_copy.wait()
    strip = min(modes, 128)

    def widen(beam_v, wide, i):
        k0 = pl.multiple_of(i * strip, strip)
        for g in range(groups):
            degree = lax.broadcasted_iota(jnp.int32, (strip, rows), 1) + g * rows
            keep = degree >= m_ref[0]
            zero = jnp.zeros((strip, rows), jnp.float32)
            b0 = jnp.where(keep, beam_v[0, pl.ds(k0, strip), g * rows:(g + 1) * rows].astype(jnp.float32), zero)
            b1 = jnp.where(keep, beam_v[1, pl.ds(k0, strip), g * rows:(g + 1) * rows].astype(jnp.float32), zero)
            wide[g, pl.ds(k0, strip), 0:rows] = b0.astype(wide.dtype)
            wide[g, pl.ds(k0, strip), rows:2 * rows] = (-b1).astype(wide.dtype)
            wide[g, pl.ds(modes + k0, strip), 0:rows] = b1.astype(wide.dtype)
            wide[g, pl.ds(modes + k0, strip), rows:2 * rows] = b0.astype(wide.dtype)

    with mark("widen"):
        loop(0, modes // strip, functools.partial(widen, beam_v, wide))
    tell("pol", pol, n_pol, meet.at[0])
    pl.semaphore_wait(meet.at[0], n_pol - 1)
    tell("freq", freq, n_freq, meet.at[1])
    pl.semaphore_wait(meet.at[1], n_freq - 1)

    if few:
        @pl.when(hub_lead)
        def _():
            await_all(noise_o, c_recv.at[1])
            inv_o[...] = 1.0 / jnp.transpose(jnp.broadcast_to(noise_o[...], (LANES, modes)))
            await_all(beam_o, c_recv.at[0])
            loop(0, modes // strip, functools.partial(widen, beam_o, wide_o))

    tile = min(modes, 256)

    def add(g, first=False):
        x = jnp.concatenate([recv[g, j].reshape(2 * rows, lanes) for j in range(splits)], axis=1)

        def body(k0):
            value = jnp.dot(wide[g, pl.ds(k0, tile), :], x, preferred_element_type=jnp.float32)
            acc[pl.ds(k0, tile), :] = value if first else acc[pl.ds(k0, tile), :] + value

        for i in range(2 * modes // tile):
            body(i * tile)

    def half(w, g, j, core):
        start = pl.multiple_of(core * block, block)
        x = jnp.concatenate([recv[g, j, c, pl.ds(start, block), :] for c in range(2)], axis=0)

        def value(k0):
            left = jnp.concatenate([w[g, k0:k0 + tile, pl.ds(pl.multiple_of(c * rows + start, block), block)]
                                    for c in range(2)], axis=1)
            return jnp.dot(left, x, preferred_element_type=jnp.float32)
        return value

    def full(w, g, j):
        x = recv[g, j].reshape(2 * rows, lanes)
        return lambda k0: jnp.dot(w[g, k0:k0 + tile, :], x, preferred_element_type=jnp.float32)

    def add_to(sums, j, product, first=False):
        for i in range(2 * modes // tile):
            at = (slice(i * tile, (i + 1) * tile), slice(j * lanes, (j + 1) * lanes))
            sums[at] = product(i * tile) if first else sums[at] + product(i * tile)

    def finish(sums, weights, j, product=None):
        power = total_ref[...]
        for i in range(2 * modes // tile):
            at = (slice(i * tile, (i + 1) * tile), slice(j * lanes, (j + 1) * lanes))
            value = sums[at]
            if product is not None:
                value = value + product(i * tile)
                sums[at] = value
            k0 = i * tile % modes
            weighted = value * value * weights[k0:k0 + tile, :]
            power = power + jnp.sum(weighted.reshape(tile // 8, 8, lanes), axis=0)
        total_ref[...] = power

    def finish_both(product, product_o):
        power, power_o = total_ref[...], jnp.zeros(total_ref.shape, jnp.float32)
        for i in range(2 * modes // tile):
            row, k0 = slice(i * tile, (i + 1) * tile), i * tile % modes
            value_o = acc_o[row, :] + product_o(i * tile)
            value = acc[row, (splits - 1) * lanes:] + product(i * tile)
            acc_o[row, :] = value_o
            acc[row, (splits - 1) * lanes:] = value
            power_o = power_o + jnp.sum((value_o * value_o * inv_o[k0:k0 + tile, :]).reshape(tile // 8, 8, lanes), axis=0)
            power = power + jnp.sum((value * value * inv_n[k0:k0 + tile, :]).reshape(tile // 8, 8, lanes), axis=0)
        total_ref[...] = power + power_o

    total_ref[...] = jnp.zeros_like(total_ref)
    if few:
        order = [pick_by(ma, [processing_order(n_ma, i)[k] for i in range(n_ma)]) for k in range(n_ma - 1)]
        last, end = order[-1], splits - 1

        def own_block(j):
            with mark(f"last{j}"):
                await_all(part(last, pol, j), z_last.at[j])

        def other_block(j):
            with mark(f"hop{j}"):
                await_all(part(last, 1 - pol, j), p_last.at[j])

        def pass_block(j, core=None, slot=None):
            at = part(last, pol if core is None else core, j)
            push(at, at, p_send.at[1], p_last.at[j if slot is None else slot], {"pol": 1 - pol})

        def take(k):
            with mark(f"wait{k}"):
                await_all(whole(order[k], pol), z_far.at[order[k]])
            for j in range(splits):
                relay(order[k], j, p_send.at[0], p_far.at[order[k]])

        def settle(source, first=False, shared=False):
            with mark("relay"):
                relayed(source)
            with mark("add"):
                add(source, first)
                if shared:
                    @pl.when(hub_lead)
                    def _():
                        add_to(acc_o, 0, full(wide_o, source, end), first)

        @pl.when(is_hub)
        def _():
            for j in range(held):
                own_block(j)
                pass_block(j)
            settle(ma, True, True)
            for j in range(held):
                other_block(j)
                add_to(acc, j, full(wide, last, j))
            for k in range(n_ma - 2):
                take(k)
                if k:
                    settle(order[k - 1], False, True)
            if n_ma > 2:
                settle(order[n_ma - 3], False, True)

        @pl.when(hub_lead)
        def _():
            with mark("y0"):
                await_all(part(last, 0, held), p_last.at[held])
            pass_block(held, 0, end)
            own_block(held)
            pass_block(held)
            for j in range(held):
                finish(acc, inv_n, j)
            finish(acc, inv_n, held, full(wide, last, held))
            with mark("y1"):
                await_all(part(last, 0, end), p_last.at[end])
            add_to(acc, end, half(wide, last, end, 0))
            add_to(acc_o, 0, half(wide_o, last, end, 0))
            own_block(end)
            finish_both(half(wide, last, end, 1), half(wide_o, last, end, 1))

        @pl.when(hub_other)
        def _():
            for j in range(held):
                finish(acc, inv_n, j)
            with mark("x"):
                await_all(part(last, 0, held), p_last.at[end])
            add_to(acc, held, half(wide, last, held, 0))
            other_block(held)
            finish(acc, inv_n, held, half(wide, last, held, 1))

        @pl.when(jnp.logical_not(is_hub))
        def _():
            before = ma
            for k in range(n_ma - 2):
                take(k)
                settle(before, k == 0)
                before = order[k]
            own_block(0)
            pass_block(0)
            settle(before)
            add_to(acc, 0, half(wide, last, 0, pol))
            for j in range(1, splits):
                own_block(j)
                pass_block(j)
                add_to(acc, j, half(wide, last, j, pol))
                other_block(j - 1)
                finish(acc, inv_n, j - 1, half(wide, last, j - 1, 1 - pol))
            other_block(end)
            finish(acc, inv_n, end, half(wide, last, end, 1 - pol))
    else:
        def pass_on(source):
            @pl.when(source != ma)
            def _():
                await_all(whole(source, pol), z_far.at[source])
                for j in range(splits):
                    relay(source, j, p_send.at[0], p_far.at[source])
        loop(0, n_ma, pass_on)
        loop(0, n_ma, relayed)
        for g in range(groups):
            add(g, g == 0)
        for j in range(splits):
            finish(acc, inv_n, j)

    row = jnp.sum(total_ref[...], axis=0, keepdims=True)
    mine[0:1, :] = row
    slots[my_slot, 0:1, :] = row
    slots[my_slot, 1:2, :] = mine[1:2, :]

    def report(r):
        pltpu.make_async_remote_copy(
            src_ref=mine, dst_ref=slots.at[my_slot], send_sem=q_send, recv_sem=q_recv,
            device_id=place(lax.rem(my_slot + r, n_all)), device_id_type=MESH).start()

    for_peers(report)
    if few:
        @pl.when(hub_lead)
        def _():
            push(acc_o, incoming, c_send.at[1], c_recv.at[0], {"pol": 0})

    with mark("drain"):
        await_all(planes.at[pl.ds(0, n_ma - 2 if few else n_ma - 1)], z_send)
        await_all(planes.at[pl.ds(0, n_ma - 1)] if few else planes, p_send.at[0])
        if few:
            await_all(planes.at[0], near_send)
            for where, count in ((hub_other, held), (jnp.logical_not(hub_other), splits)):
                @pl.when(where)
                def _():
                    await_all(planes.at[0, pl.ds(0, count)], p_send.at[1])

            @pl.when(hub_lead)
            def _():
                await_all(extra, c_send.at[0])

            @pl.when(has_guest)
            def _():
                await_all(guest, g_send)

            @pl.when(hub_other)
            def _():
                await_all(beam_o, c_send.at[0])
                await_all(noise_o, c_send.at[1])
                with mark("incoming"):
                    await_all(incoming, c_recv.at[0])
                acc[:, end * lanes:] = incoming[...]
    with mark("heard"):
        await_all(slots.at[pl.ds(0, n_all - 1)], q_recv)

    per_freq = n_ma * n_pol
    tail = mark('tail'); tail.__enter__()
    masked, live, here = 0.0, 0.0, 0.0
    for f in range(n_freq):
        channel = jnp.sum(jnp.sum(slots[f * per_freq:(f + 1) * per_freq, 0, :], axis=0, keepdims=True), axis=1, keepdims=True) / total
        flag = slots[f * per_freq, 1:2, 0:1]
        masked += flag * channel
        live += flag
        here += jnp.where(freq == f, channel, 0.0)
    band = masked / live
    factor = mine[1:2, 0:1] / jnp.sqrt(0.5 * here + 0.5 * band + 1e-06)
    power_ref[...] = jnp.broadcast_to(here, power_ref.shape)
    scale_ref[...] = rs_n[...] * factor
    await_all(slots.at[pl.ds(0, n_all - 1)], q_send)
    if few:
        @pl.when(hub_lead)
        def _():
            await_all(acc_o, c_send.at[1])
    tail.__exit__(None,None,None)


def rescale_kernel(acc, scale_ref, power_ref, out_ref, channel_ref, staged, channel, sems, channel_sem):
    modes = scale_ref.shape[0]
    columns = acc.shape[1]
    strip = modes // sems.shape[0]
    channel[0] = power_ref[0, 0]
    last = pltpu.make_async_copy(channel, channel_ref, channel_sem)
    copies = []
    for i in range(sems.shape[0]):
        k0 = i * strip
        scale = scale_ref[k0:k0 + strip, :]
        for c in range(2):
            for j in range(columns // LANES):
                value = acc[c * modes + k0:c * modes + k0 + strip, j * LANES:(j + 1) * LANES]
                staged[c, k0:k0 + strip, j * LANES:(j + 1) * LANES] = (value * scale).astype(staged.dtype)
        copies.append(pltpu.make_async_copy(
            staged.at[:, pl.ds(k0, strip)], out_ref.at[:, pl.ds(k0, strip)], sems.at[i]))
        copies[-1].start()
        if i == 0:
            last.start()
    for copy in copies:
        copy.wait()
    last.wait()


def on_device(sizes, alm, beam, m_table, chan_mask, noise):
    n_ma, n_freq, n_pol = sizes
    coeffs = alm[:, 0]
    response = beam[0, 0]
    block, columns = coeffs.shape[1], coeffs.shape[3]
    modes, degrees = response.shape[1], response.shape[2]
    per_source = n_pol * block
    rows = per_source * max(1, min(n_ma, 256 // per_source))
    groups = degrees // rows
    splits = columns // LANES
    n_all = n_ma * n_freq * n_pol
    total = float(n_ma * modes * n_pol * columns)
    vmem = pl.BlockSpec(memory_space=pltpu.VMEM)
    hbm = pl.BlockSpec(memory_space=pltpu.HBM)
    smem = pl.BlockSpec(memory_space=pltpu.SMEM)
    dma = pltpu.SemaphoreType.DMA
    keep = functools.partial(pltpu.with_memory_space_constraint, memory_space=pltpu.HBM)
    visibility, scale, power = pl.pallas_call(
        functools.partial(step_kernel, sizes, total),
        out_shape=(
            jax.ShapeDtypeStruct((2 * modes, columns), jnp.float32),
            jax.ShapeDtypeStruct((modes, LANES), jnp.float32),
            jax.ShapeDtypeStruct((1, LANES), jnp.float32),
        ),
        in_specs=[hbm, hbm, smem, smem, hbm],
        out_specs=(vmem, vmem, vmem),
        scratch_shapes=[
            pltpu.VMEM((2, block, n_ma, columns), jnp.bfloat16),
            pltpu.VMEM((n_ma, splits, 2, block, LANES), jnp.bfloat16),
            pltpu.VMEM((2, 2, block, LANES), jnp.bfloat16),
            pltpu.VMEM((block, LANES), jnp.bfloat16),
            pltpu.VMEM((groups, splits, 2, rows, LANES), jnp.bfloat16),
            pltpu.VMEM((groups, 2 * modes, 2 * rows), jnp.bfloat16),
            pltpu.VMEM((groups, 2 * modes, 2 * rows), jnp.bfloat16),
            pltpu.VMEM((2, modes, degrees), jnp.bfloat16),
            pltpu.VMEM((2, modes, degrees), jnp.bfloat16),
            pltpu.VMEM((2 * modes, LANES), jnp.float32),
            pltpu.VMEM((2 * modes, LANES), jnp.float32),
            pltpu.VMEM((modes, LANES), jnp.float32),
            pltpu.VMEM((modes, LANES), jnp.float32),
            pltpu.VMEM((modes, LANES), jnp.float32),
            pltpu.VMEM((2, LANES), jnp.float32),
            pltpu.VMEM((n_all, 2, LANES), jnp.float32),
            pltpu.VMEM((8, LANES), jnp.float32),
            pltpu.VMEM((1, modes), jnp.float32),
            pltpu.VMEM((1, modes), jnp.float32),
            dma, dma, dma, dma, dma((2,)), dma((3,)), dma((n_ma,)), dma((splits,)), dma((2,)), dma((n_ma,)), dma((splits,)),
            dma((splits,)), dma, dma, dma,
            pltpu.SemaphoreType.REGULAR((2,)), pltpu.SemaphoreType.REGULAR((2,)), dma,
        ],
        compiler_params=pltpu.CompilerParams(collective_id=0, has_side_effects=True, vmem_limit_bytes=40 * 1024 * 1024),
        name="driftscan_step",
    )(keep(coeffs), keep(response), m_table, chan_mask, keep(noise))
    pieces = 8 if modes % 128 == 0 else 1
    scaled, channel_power = pl.pallas_call(
        rescale_kernel,
        out_shape=(
            jax.ShapeDtypeStruct((2, modes, columns), jnp.bfloat16),
            jax.ShapeDtypeStruct((1,), jnp.float32),
        ),
        in_specs=[vmem, vmem, vmem],
        out_specs=(hbm, hbm),
        scratch_shapes=[pltpu.VMEM((2, modes, columns), jnp.bfloat16), pltpu.SMEM((1,), jnp.float32), dma((pieces,)), dma],
        compiler_params=pltpu.CompilerParams(vmem_limit_bytes=16 * 1024 * 1024),
        name="rescale",
    )(visibility, scale, power)
    return scaled[:, None, None], channel_power


def solution(mesh):
    sizes = (mesh.shape["ma"], mesh.shape["freq"], mesh.shape["pol"])
    return jax.shard_map(
        functools.partial(on_device, sizes),
        mesh=mesh,
        in_specs=(
            P(None, "freq", ("ma", "pol"), None, "sky"),
            P("ma", "freq", None, "pol", None),
            P("ma"),
            P("freq"),
            P("freq", "pol"),
        ),
        out_specs=(P(None, "freq", "ma", "pol", "sky"), P(("sky", "freq"))),
        check_vma=False,
    )
```
